512 devices in a mesh: seq: 64 (over z, y), head: 4 (over x), rep: 2 (over core).
Axes of the slice: x: 4, y: 8, z: 8, core: 2. Of those that a mesh axis runs over, the one named last changes fastest.
Arguments:
- queries: bfloat16 [16384, 8, 128], P(('rep', 'seq'), 'head'), parts along dimension 0, may hold values from -8 to 8
- keys: bfloat16 [16384, 128], P(('rep', 'seq')), parts along dimension 0, may hold values from -8 to 8
- values: bfloat16 [16384, 128], P(('rep', 'seq')), parts along dimension 0, may hold values from -6 to 6
- query_weight: float32 [16, 64, 128], P(('rep', 'head')), parts along dimension 0, may hold values from -0.075 to 0.075
- key_weight: float32 [16, 64, 128], P(('rep', 'head')), parts along dimension 0, may hold values from -0.075 to 0.075
Outputs:
- loss: float32 [2], P('rep'), parts along dimension 0
- grad_query_weight: float32 [16, 64, 128], P(('rep', 'head')), parts along dimension 0
- grad_key_weight: float32 [16, 64, 128], P(('rep', 'head')), parts along dimension 0
The draws below stay inside these ranges and needn't reach their ends.
There are 2 independent parts, one for each index of `rep`. The reference program is written for one: setup_inputs(seed, part) draws one part's arguments, and reference() takes and returns one part's arrays. A program takes and returns all parts, laid end to end along the dimension named above; each array names one. Nothing has to cross between parts.
All inputs are finite; a program needn't handle non-finite values.
Results may differ from the reference program's by a relative error of at most 0.00045.
Values may be sent and summed in bfloat16 or wider, within the bound.
A program may use at most 64 MiB of HBM per device.

```python
import math
import jax
import jax.numpy as jnp
from jax import lax

DH = 128
HEADS = 8
FH = 64
WINDOW = 64
TOK_DEV = 128
TOKENS = 8192


def drawn_pair(key):
    base = jax.random.fold_in(key, 4242)
    pick_query, pick_key = jax.random.split(base, 2)
    queries = 1.7 * jax.random.truncated_normal(pick_query, -4.5, 4.5, (TOKENS, HEADS, DH), jnp.float32)
    keys = 1.7 * jax.random.truncated_normal(pick_key, -4.5, 4.5, (TOKENS, DH), jnp.float32)
    return (queries, keys)


def draw_queries(key, part):
    return drawn_pair(key)[0].astype(jnp.bfloat16)


def draw_keys(key, part):
    return drawn_pair(key)[1].astype(jnp.bfloat16)


def shard_levels(own_key, dims, shards, smallest, high):
    gain = 1.0
    for axis_at, parts in shards:
        heights = jax.random.uniform(jax.random.fold_in(jax.random.fold_in(own_key, 6), axis_at), (parts,), jnp.float32, smallest / len(shards), high / len(shards))
        gain = gain * jnp.repeat(jnp.exp(heights), dims[axis_at] // parts).reshape((-1,) + (1,) * (len(dims) - 1 - axis_at))
    return gain


def gaussian(own_key, dims, spread, reach, cuts=(), kind=jnp.bfloat16):
    loudness = shard_levels(own_key, dims, cuts, -0.22, 0.18) if cuts else 1.0
    drawn = jax.random.normal(own_key, dims, jnp.float32) * spread * loudness
    return jnp.minimum(jnp.maximum(drawn, -reach), reach).astype(kind)


def setup_inputs(seed: int = 0, part: int = 0) -> dict:
    streams_of = jax.random.split(jax.random.key(seed), 6)
    own_keys = jax.random.split(jax.random.fold_in(streams_of[5], part), 6)
    return {
        "queries": draw_queries(jax.random.fold_in(jax.random.fold_in(streams_of[5], part), 71), part),
        "keys": draw_keys(jax.random.fold_in(jax.random.fold_in(streams_of[5], part), 71), part),
        "values": gaussian(own_keys[2], (TOKENS, DH), 1.0, 6.0, ((0, 64),)),
        "query_weight": jnp.clip(jax.random.uniform(own_keys[3], (HEADS, FH, DH), jnp.float32, -0.075, 0.075) * shard_levels(own_keys[3], (HEADS, FH, DH), ((0, 4),), -0.4, 0.0), -0.075, 0.075),
        "key_weight": jnp.clip(jax.random.uniform(own_keys[4], (HEADS, FH, DH), jnp.float32, -0.075, 0.075) * shard_levels(own_keys[4], (HEADS, FH, DH), ((0, 4),), -0.4, 0.0), -0.075, 0.075),
    }


very_low = -1.0e30
exact = lax.Precision.HIGHEST


def feature_map(act):
    first = jnp.exp(act)
    second = jnp.exp(-act)
    return jnp.concatenate([first / jnp.sum(first, axis=-1, keepdims=True), second / jnp.sum(second, axis=-1, keepdims=True)], axis=-1)


def feature_back(features, grad):
    half = features.shape[-1] // 2
    first = features[..., :half]
    second = features[..., half:]
    grad_first = grad[..., :half]
    grad_second = grad[..., half:]
    return first * (grad_first - jnp.sum(first * grad_first, axis=-1, keepdims=True)) - second * (grad_second - jnp.sum(second * grad_second, axis=-1, keepdims=True))


def rounded(array):
    return lax.optimization_barrier(array.astype(jnp.bfloat16)).astype(jnp.float32)


def reference(queries, keys, values, query_weight, key_weight):
    width = queries.shape[2]
    scale = width ** -0.5
    block = math.gcd(TOK_DEV, 128)
    queries_wide = queries.astype(jnp.float32)
    keys_wide = keys.astype(jnp.float32)
    values_wide = values.astype(jnp.float32)
    key_features = feature_map(jnp.einsum('jd,hfd->hjf', keys_wide, key_weight, precision=exact))
    key_place = jnp.arange(TOKENS, dtype=jnp.int32)

    def one_block(carry, start):
        loss_sum, key_grad, query_grad = carry
        query_block = lax.dynamic_slice_in_dim(queries_wide, start, block, 0)
        query_place = start + jnp.arange(block, dtype=jnp.int32)
        scores = jnp.einsum('thd,jd->htj', query_block, keys_wide, precision=exact) * scale
        causal = (key_place[None, :] <= query_place[:, None])[None]
        teacher_best = jnp.max(jnp.where(causal, scores, very_low), axis=-1)
        teacher_weights = jnp.where(causal, jnp.exp(scores - teacher_best[..., None]), 0.0)
        teacher_total = jnp.sum(teacher_weights, axis=-1)
        teacher_sum = jnp.einsum('htj,jd->htd', rounded(teacher_weights), values_wide, precision=exact)
        teacher = rounded(teacher_sum / teacher_total[..., None])
        window = causal & (key_place[None, :] > query_place[:, None] - WINDOW)[None]
        linear_mask = (key_place[None, :] <= query_place[:, None] - WINDOW)[None]
        window_best = jnp.max(jnp.where(window, scores, very_low), axis=-1)
        window_weights = jnp.where(window, jnp.exp(scores - window_best[..., None]), 0.0)
        window_total = jnp.sum(window_weights, axis=-1)
        window_sum = jnp.einsum('htj,jd->htd', rounded(window_weights), values_wide, precision=exact)
        query_features = feature_map(jnp.einsum('thd,hfd->htf', query_block, query_weight, precision=exact))
        linear = jnp.where(linear_mask, jnp.einsum('htf,hjf->htj', query_features, key_features, precision=exact), 0.0)
        linear_sum = jnp.einsum('htj,jd->htd', linear, values_wide, precision=exact)
        linear_total = jnp.sum(linear, axis=-1)
        lift = jnp.exp(-window_best)
        denominator = window_total + lift * linear_total
        student = (window_sum + lift[..., None] * linear_sum) / denominator[..., None]
        difference = student - teacher
        loss_sum = loss_sum + jnp.sum(difference * difference) / TOKENS
        grad_out = 2.0 * difference / TOKENS
        num_grad = lift[..., None] * grad_out / denominator[..., None]
        den_grad = -lift * jnp.sum(grad_out * student, axis=-1) / denominator
        link = jnp.where(linear_mask, jnp.einsum('htd,jd->htj', num_grad, values_wide, precision=exact) + den_grad[..., None], 0.0)
        query_feature_grad = jnp.einsum('htj,hjf->htf', link, key_features, precision=exact)
        key_grad = key_grad + jnp.einsum('htj,htf->hjf', link, query_features, precision=exact)
        query_act_grad = feature_back(query_features, query_feature_grad)
        query_grad = query_grad + jnp.einsum('htf,thd->hfd', query_act_grad, query_block, precision=exact)
        return (loss_sum, key_grad, query_grad), None

    init = (jnp.zeros((), jnp.float32), jnp.zeros(key_features.shape, jnp.float32), jnp.zeros(query_weight.shape, jnp.float32))
    starts = jnp.arange(0, TOKENS, block, dtype=jnp.int32)
    (loss_sum, key_grad, query_grad), unused = lax.scan(one_block, init, starts)
    key_act_grad = feature_back(key_features, key_grad)
    grad_key = jnp.einsum('hjf,jd->hfd', key_act_grad, keys_wide, precision=exact)
    return loss_sum.reshape(1), query_grad, grad_key
```

```python
import functools

import jax
import jax.numpy as jnp
from jax import lax
from jax.experimental import pallas as pl
from jax.experimental.pallas import tpu as pltpu
from jax.sharding import Mesh
from jax.sharding import PartitionSpec as P

WINDOW = 64
Z, Y, X = "seq_0", "seq_1", "head"
REP_SEQ = ("rep", Z, Y)
MESH = pl.DeviceIdType.MESH
RING = 8
LOW = -1e30
F32 = jnp.float32
BF16 = jnp.bfloat16
CHUNK = 4
FAR_FIRST = (4, 3, 5, 2, 6, 1, 7)


def around(place, steps):
    return lax.rem(place + (steps + RING), RING)


def remote(src, dst, send, recv, axis, place):
    return pltpu.make_async_remote_copy(
        src_ref=src,
        dst_ref=dst,
        send_sem=send,
        recv_sem=recv,
        device_id={axis: place},
        device_id_type=MESH,
    )


def greet(peers):
    barrier = pltpu.get_barrier_semaphore()
    for axis, place in peers:
        pl.semaphore_signal(barrier, inc=1, device_id={axis: place}, device_id_type=MESH)
    pl.semaphore_wait(barrier, len(peers))


def gather_kernel(k_ref, v_ref, kb, vb, send_sems, k_recv, v_recv):
    z, y = lax.axis_index(Z), lax.axis_index(Y)
    greet([(Z, around(z, 1)), (Z, around(z, -1)), (Y, around(y, 1)), (Y, around(y, -1))])
    place = {Z: z, Y: y}
    streams = (
        (k_ref, kb, send_sems.at[0], k_recv, Y, Z),
        (v_ref, vb, send_sems.at[1], v_recv, Z, Y),
    )

    def index(stream, along, across):
        at = {stream[4]: around(place[stream[4]], along), stream[5]: around(place[stream[5]], across)}
        return at[Z] * RING + at[Y]

    def send(stream, src, at, axis, step):
        remote(src, stream[1].at[at], stream[2], stream[3].at[at], axis, around(place[axis], step)).start()

    def arrived(stream, at):
        block = stream[1].at[at]
        remote(block, block, stream[2], stream[3].at[at], Z, z).wait_recv()

    for stream in streams:
        own = index(stream, 0, 0)
        for axis in (stream[4], stream[5]):
            send(stream, stream[0], own, axis, 1)
            send(stream, stream[0], own, axis, -1)
    for stream in streams:
        stream[1][index(stream, 0, 0)] = stream[0][...]
    for hop in range(1, 5):
        for way in (1, -1):
            if hop == 4 and way == -1:
                continue
            for stream in streams:
                at = index(stream, -way * hop, 0)
                arrived(stream, at)
                if hop < (4 if way == 1 else 3):
                    send(stream, stream[1].at[at], at, stream[4], way)
                send(stream, stream[1].at[at], at, stream[5], 1)
                send(stream, stream[1].at[at], at, stream[5], -1)
    for hop in range(1, 5):
        for along in (0, -1, 1, -2, 2, -3, 3, 4):
            for way in (1, -1):
                last = (way == 1) == (along % 2 == 0)
                if hop == 4 and not last:
                    continue
                for stream in streams:
                    at = index(stream, along, -way * hop)
                    arrived(stream, at)
                    if hop < 3 or (hop == 3 and last):
                        send(stream, stream[1].at[at], at, stream[5], way)
    for stream in streams:
        sent = stream[1].at[pl.ds(0, RING * RING - 1)]
        remote(sent, sent, stream[2], stream[3].at[0], Z, z).wait_send()


VMEM = pl.BlockSpec(memory_space=pltpu.VMEM)


def gather(keys, values):
    blocks = jax.ShapeDtypeStruct((RING * RING, *keys.shape), BF16)
    return pl.pallas_call(
        gather_kernel,
        out_shape=(blocks, blocks),
        in_specs=[VMEM] * 2,
        out_specs=(VMEM, VMEM),
        scratch_shapes=[
            pltpu.SemaphoreType.DMA((2,)),
            pltpu.SemaphoreType.DMA((RING * RING,)),
            pltpu.SemaphoreType.DMA((RING * RING,)),
        ],
        compiler_params=pltpu.CompilerParams(collective_id=0, has_side_effects=True),
        name="gather_kv",
    )(keys, values)


def exchange_kernel(scan, rows, tile, *refs):
    if tile:
        x_ref, tile_ref, out, tile_out, b1, t, b2, o, tiles, send, r1, r2, r3, rt = refs
    else:
        x_ref, out, b1, t, b2, o, send, r1, r2, r3 = refs
    z, y = lax.axis_index(Z), lax.axis_index(Y)
    peers = [(Y, around(y, d)) for d in FAR_FIRST] + [(Z, around(z, d)) for d in FAR_FIRST]
    if tile:
        x = lax.axis_index(X)
        others = [lax.rem(x + d, 4) for d in (2, 1, 3)]
        peers += [(X, p) for p in others]
    greet(peers)
    for d in FAR_FIRST:
        p = around(y, d)
        remote(x_ref.at[p], b1.at[y], send.at[0], r1.at[y], Y, p).start()
    if tile:
        for p in others:
            remote(tile_ref, tiles.at[x], send.at[3], rt.at[x], X, p).start()
    b1[y] = x_ref[y]
    for d in (1, 7, 2, 6, 3, 5, 4):
        p = around(y, d)
        remote(b1.at[p], b1.at[p], send.at[0], r1.at[p], Y, p).wait_recv()
    total = b1[0]
    for k in range(1, RING):
        total = total + b1[k]
    t[...] = total
    for d in FAR_FIRST:
        p = around(z, d)
        remote(t, b2.at[z], send.at[1], r2.at[z], Z, p).start()
    b2[z] = total
    for d in (1, 7, 2, 6, 3, 5, 4):
        p = around(z, d)
        remote(b2.at[p], b2.at[p], send.at[1], r2.at[p], Z, p).wait_recv()
    if scan:
        base = jnp.zeros((scan, 128), F32)
        for k in range(RING):
            base = base + jnp.where(k > z, b2[k, :scan], 0.0)
        for k in reversed(range(RING)):
            o[k, :scan] = base
            base = base + b1[k, :scan]
    total = b2[0, scan:]
    for k in range(1, RING):
        total = total + b2[k, scan:]
    for k in range(RING):
        o[k, scan:] = total
    for d in FAR_FIRST:
        p = around(y, d)
        remote(o.at[p], out.at[y], send.at[2], r3.at[y], Y, p).start()
    out[y] = o[y]
    if tile:
        tiles[x] = tile_ref[...]
        for p in others:
            remote(tile_ref, tiles.at[p], send.at[3], rt.at[p], X, p).wait_recv()
        tile_out[...] = tiles[0] + tiles[1] + tiles[2] + tiles[3]
    for d in (1, 7, 2, 6, 3, 5, 4):
        p = around(y, d)
        remote(out.at[p], out.at[p], send.at[2], r3.at[p], Y, p).wait_recv()
    most = x_ref.at[pl.ds(0, RING - 1)]
    for k in range(3):
        remote(most, most, send.at[k], r1.at[0], Y, y).wait_send()
    if tile:
        three = tiles.at[pl.ds(0, 3)]
        remote(three, three, send.at[3], r1.at[0], Y, y).wait_send()


def exchange(x, scan, collective_id, tile=None):
    rows = x.shape[1]
    full = pltpu.VMEM((RING, rows, 128), F32)
    dma = pltpu.SemaphoreType.DMA
    scratch = [full, pltpu.VMEM((rows, 128), F32), full, full]
    sems = [dma((4,)), dma((RING,)), dma((RING,)), dma((RING,))]
    outs = [jax.ShapeDtypeStruct(x.shape, F32)]
    args = [x]
    if tile is not None:
        scratch.append(pltpu.VMEM((4, 8, 128), F32))
        sems.append(dma((4,)))
        outs.append(jax.ShapeDtypeStruct((8, 128), F32))
        args.append(tile)
    return pl.pallas_call(
        functools.partial(exchange_kernel, scan, rows, tile is not None),
        out_shape=tuple(outs),
        in_specs=[VMEM] * len(args),
        out_specs=(VMEM,) * len(outs),
        scratch_shapes=scratch + sems,
        compiler_params=pltpu.CompilerParams(collective_id=collective_id, has_side_effects=True),
        name="exchange",
    )(*args)


NN = (((1,), (0,)), ((), ()))
NT = (((1,), (1,)), ((), ()))


def dot(a, b, dims=NN):
    return lax.dot_general(a, b, dims, preferred_element_type=F32)


def two(a):
    high = a.astype(BF16)
    return high, (a - high.astype(F32)).astype(BF16)


def dot_wide(a, b, dims=NN):
    a_high, a_low = two(a)
    b_high, b_low = two(b)
    return dot(a_high, b_high, dims) + (dot(a_high, b_low, dims) + dot(a_low, b_high, dims))


def dot_left(a, b, dims=NN):
    high, low = two(a)
    return dot(high, b, dims) + dot(low, b, dims)


def dot_right(a, b, dims=NN):
    high, low = two(b)
    return dot(a, high, dims) + dot(a, low, dims)


def three(a):
    high = a.astype(BF16)
    rest = a - high.astype(F32)
    mid = rest.astype(BF16)
    return high, mid, (rest - mid.astype(F32)).astype(BF16)


def features_of(pieces, tokens):
    act = dot(pieces[0], tokens, NT) + (dot(pieces[1], tokens, NT) + dot(pieces[2], tokens, NT))
    half = 64
    parts = []
    for h in range(act.shape[0] // half):
        one = act[h * half : (h + 1) * half]
        for e in (jnp.exp(one), jnp.exp(-one)):
            parts.append(e * (1.0 / jnp.sum(e, axis=0, keepdims=True)))
    return jnp.concatenate(parts, axis=0)


def features_back(features, grad):
    half = features.shape[0] // 2
    p, r = features[:half], features[half:]
    dp, dr = grad[:half], grad[half:]
    return p * (dp - jnp.sum(p * dp, axis=0, keepdims=True)) - r * (
        dr - jnp.sum(r * dr, axis=0, keepdims=True)
    )


def iota(shape, axis):
    return lax.broadcasted_iota(jnp.int32, shape, axis)


def attend_kernel(
    q_ref, kb, vb, wq_ref, wk_ref,
    x_out, tile_out, kf_out, kfg_out, kext_out, vext_out,
    scores, best, state, state_sum, total, accum,
):
    z, y = lax.axis_index(Z), lax.axis_index(Y)
    me = z * RING + y
    rows = 128
    tokens = rows * RING * RING
    first = me * rows
    bound = first - WINDOW
    scale = 128 ** (-0.5)
    q_all = q_ref[...].reshape(2 * rows, 128)
    wide = CHUNK * rows
    count = me // CHUNK + 1
    wk = three(wk_ref[...].reshape(128, 128))

    best[...] = jnp.full(best.shape, LOW, F32)
    state[...] = jnp.zeros_like(state)
    state_sum[...] = jnp.zeros_like(state_sum)
    total[...] = jnp.zeros_like(total)
    accum[...] = jnp.zeros_like(accum)

    query_place = first + jnp.bitwise_and(iota((2 * rows, wide), 0), rows - 1)
    lane = iota((2 * rows, wide), 1)

    def lanes(fold, start, value):
        for k in range(CHUNK):
            start = fold(start, value[:, k * 128 : (k + 1) * 128])
        return start

    @pl.loop(0, count)
    def _(c):
        kc = kb[pl.ds(c * CHUNK, CHUNK)].reshape(wide, 128)
        vc = vb[pl.ds(c * CHUNK, CHUNK)].reshape(wide, 128)
        s = dot(q_all, kc, NT) * scale
        s = jnp.where(lane + c * wide <= query_place, s, LOW)
        scores[c] = s
        best[...] = lanes(jnp.maximum, best[...], s)
        f = features_of(wk, kc)
        f = jnp.where(lane + c * wide < bound, f, 0.0)
        state_sum[...] = lanes(jnp.add, state_sum[...], f)
        state[...] += dot_left(f, vc)

    top = jnp.max(best[...], axis=1, keepdims=True)

    @pl.loop(0, count)
    def _(c):
        vc = vb[pl.ds(c * CHUNK, CHUNK)].reshape(wide, 128)
        w = jnp.exp(scores[c] - top)
        total[...] = lanes(jnp.add, total[...], w)
        accum[...] += dot(w.astype(BF16), vc)

    teacher = accum[...] / jnp.sum(total[...], axis=1, keepdims=True)
    teacher = teacher.astype(BF16).astype(F32)

    before = jnp.maximum(me - 1, 0)
    kext = jnp.concatenate([kb[before], kb[me]], axis=0)
    vext = jnp.concatenate([vb[before], vb[me]], axis=0)
    kf_all = features_of(wk, kext)
    kf_out[...] = kf_all
    kext_out[...] = kext
    vext_out[...] = vext
    span = 2 * rows
    t_place = first + iota((rows, span), 0)
    j_place = first - rows + iota((rows, span), 1)
    window = (j_place <= t_place) & (j_place > t_place - WINDOW) & (j_place >= 0)
    linear_mask = (j_place <= t_place - WINDOW) & (j_place >= bound) & (j_place >= 0)
    t_turned = first + iota((span, rows), 1)
    j_turned = first - rows + iota((span, rows), 0)
    turned_mask = (j_turned <= t_turned - WINDOW) & (j_turned >= bound) & (j_turned >= 0)

    loss = jnp.zeros((8, 128), F32)
    rows_of_a = []
    for h in range(2):
        q = q_ref[h]
        s = dot(q, kext, NT) * scale
        window_best = jnp.max(jnp.where(window, s, LOW), axis=1, keepdims=True)
        weights = jnp.where(window, jnp.exp(s - window_best), 0.0)
        window_total = jnp.sum(weights, axis=1, keepdims=True)
        window_sum = dot(weights.astype(BF16), vext)
        qft = features_of(three(wq_ref[h]), q)
        qf = qft.T
        kft = kf_all[h * 128 : (h + 1) * 128]
        prefix = state[h * 128 : (h + 1) * 128, :]
        prefix_sum = jnp.sum(state_sum[h * 128 : (h + 1) * 128, :], axis=1, keepdims=True)
        linear = jnp.where(linear_mask, dot_wide(qf, kft), 0.0)
        linear_sum = dot_left(linear, vext) + dot_wide(qf, prefix)
        linear_total = jnp.sum(linear, axis=1, keepdims=True) + dot_wide(
            qf, jnp.broadcast_to(prefix_sum, (128, 128))
        )
        lift = jnp.exp(-window_best)
        inverse = 1.0 / (window_total + lift * linear_total)
        student = (window_sum + lift * linear_sum) * inverse
        difference = student - teacher[h * rows : (h + 1) * rows]
        square = difference * difference
        for k in range(rows // 8):
            loss = loss + square[k * 8 : (k + 1) * 8]
        grad_out = difference * (2.0 / tokens)
        num_grad = lift * grad_out * inverse
        den_grad = -lift * jnp.sum(grad_out * student, axis=1, keepdims=True) * inverse
        ngt = num_grad.T
        dgt = den_grad.T
        link = jnp.where(turned_mask, dot_right(vext, ngt) + dgt[:1], 0.0)
        qfg = dot_wide(kft, link) + dot_wide(prefix, ngt) + prefix_sum * dgt[:1]
        kfg_out[h * 128 : (h + 1) * 128] = dot_wide(qft, link, NT)
        adjoint = dot_wide(ngt, qft, NT)
        for k in range(4):
            x_out[4 * h + k, 0:32] = adjoint[32 * k : 32 * (k + 1)]
        rows_of_a.append(dot_wide(dgt[:8], qft, NT))
        grad_query = dot_left(features_back(qft, qfg), q)
        for k in range(4):
            x_out[4 * h + k, 40:56] = grad_query[16 * k : 16 * (k + 1)]
    tile_out[...] = loss
    pair = jnp.where(iota((8, 128), 0) == 0, rows_of_a[0], rows_of_a[1])
    for k in range(RING):
        x_out[k, 32:40] = pair


def attend(q, kb, vb, wq, wk):
    shape = jax.ShapeDtypeStruct
    big = pltpu.VMEM((256, 128), F32)
    return pl.pallas_call(
        attend_kernel,
        out_shape=(
            shape((RING, 56, 128), F32),
            shape((8, 128), F32),
            shape((256, 256), F32),
            shape((256, 256), F32),
            shape((256, 128), BF16),
            shape((256, 128), BF16),
        ),
        in_specs=[VMEM] * 5,
        out_specs=(VMEM,) * 6,
        scratch_shapes=[
            pltpu.VMEM((RING * RING // CHUNK, 256, CHUNK * 128), F32),
            big, big, big, big, big,
        ],
        name="attend",
    )(q, kb, vb, wq, wk)


def key_grad_kernel(x_ref, tile_ref, kf_ref, kfg_ref, kext_ref, vext_ref, out):
    z, y = lax.axis_index(Z), lax.axis_index(Y)
    me = z * RING + y
    at = iota((1, 256), 1)
    covered = (at >= WINDOW) & (at < WINDOW + 128) & (me * 128 - 128 + at >= 0)
    kext, vext = kext_ref[...], vext_ref[...]
    for h in range(2):
        later = x_ref[4 * h : 4 * h + 4, 0:32].reshape(128, 128)
        add = dot_right(vext, later) + x_ref[0, 32 + h : 33 + h]
        grad = kfg_ref[h * 128 : (h + 1) * 128] + add.T
        grad = jnp.where(covered, grad, 0.0)
        grad_key = dot_left(features_back(kf_ref[h * 128 : (h + 1) * 128], grad), kext)
        for k in range(4):
            out[4 * h + k, 0:16] = grad_key[16 * k : 16 * (k + 1)]
    for k in range(RING):
        out[k, 16:24] = tile_ref[...]


def key_grad(*args):
    return pl.pallas_call(
        key_grad_kernel,
        out_shape=jax.ShapeDtypeStruct((RING, 24, 128), F32),
        in_specs=[VMEM] * len(args),
        out_specs=VMEM,
        name="key_grad",
    )(*args)


def local(queries, keys, values, query_weight, key_weight):
    tokens = queries.shape[0] * RING * RING
    q = jnp.transpose(queries, (1, 0, 2))
    kb, vb = gather(keys, values)
    x, tile, kf, kfg, kext, vext = attend(q, kb, vb, query_weight, key_weight)
    sums, tile = exchange(x, 40, 1, tile)
    last = exchange(key_grad(sums, tile, kf, kfg, kext, vext), 0, 2)[0]
    grad_query = sums[:, 40:56].reshape(2, 64, 128)
    grad_key = last[:, 0:16].reshape(2, 64, 128)
    loss = (jnp.sum(last[0, 16:24]) / tokens).reshape(1)
    return loss, grad_query, grad_key


def solution(mesh):
    split = Mesh(
        mesh.devices.reshape(8, 8, mesh.shape["head"], mesh.shape["rep"]),
        (Z, Y, X, "rep"),
    )
    return jax.shard_map(
        local,
        mesh=split,
        in_specs=(
            P(REP_SEQ, X, None),
            P(REP_SEQ, None),
            P(REP_SEQ, None),
            P(("rep", X), None, None),
            P(("rep", X), None, None),
        ),
        out_specs=(P("rep"), P(("rep", X), None, None), P(("rep", X), None, None)),
        check_vma=False,
    )
```

```python
import functools

import jax
import jax.numpy as jnp
from jax import lax
from jax.experimental import pallas as pl
from jax.experimental.pallas import tpu as pltpu
from jax.sharding import Mesh
from jax.sharding import PartitionSpec as P

WINDOW = 64
Z, Y, X = "seq_0", "seq_1", "head"
REP_SEQ = ("rep", Z, Y)
MESH = pl.DeviceIdType.MESH
RING = 8
LOW = -1e30
F32 = jnp.float32
BF16 = jnp.bfloat16
FAR_FIRST = (4, 3, 5, 2, 6, 1, 7)


def around(place, steps):
    return lax.rem(place + (steps + RING), RING)


def remote(src, dst, send, recv, axis, place):
    return pltpu.make_async_remote_copy(
        src_ref=src,
        dst_ref=dst,
        send_sem=send,
        recv_sem=recv,
        device_id={axis: place},
        device_id_type=MESH,
    )


def greet(peers):
    barrier = pltpu.get_barrier_semaphore()
    for axis, place in peers:
        pl.semaphore_signal(barrier, inc=1, device_id={axis: place}, device_id_type=MESH)
    pl.semaphore_wait(barrier, len(peers))


NN = (((1,), (0,)), ((), ()))
NT = (((1,), (1,)), ((), ()))


def dot(a, b, dims=NN):
    return lax.dot_general(a, b, dims, preferred_element_type=F32)


def two(a):
    high = a.astype(BF16)
    return high, (a - high.astype(F32)).astype(BF16)


def dot_wide(a, b, dims=NN):
    a_high, a_low = two(a)
    b_high, b_low = two(b)
    return dot(a_high, b_high, dims) + (dot(a_high, b_low, dims) + dot(a_low, b_high, dims))


def dot_left(a, b, dims=NN):
    high, low = two(a)
    return dot(high, b, dims) + dot(low, b, dims)


def dot_right(a, b, dims=NN):
    high, low = two(b)
    return dot(a, high, dims) + dot(a, low, dims)


def three(a):
    high = a.astype(BF16)
    rest = a - high.astype(F32)
    mid = rest.astype(BF16)
    return high, mid, (rest - mid.astype(F32)).astype(BF16)


def features_of(pieces, tokens):
    act = dot(pieces[0], tokens, NT) + (dot(pieces[1], tokens, NT) + dot(pieces[2], tokens, NT))
    half = 64
    parts = []
    for h in range(act.shape[0] // half):
        one = act[h * half : (h + 1) * half]
        for e in (jnp.exp(one), jnp.exp(-one)):
            parts.append(e * (1.0 / jnp.sum(e, axis=0, keepdims=True)))
    return jnp.concatenate(parts, axis=0)


def features_back(features, grad):
    half = features.shape[0] // 2
    p, r = features[:half], features[half:]
    dp, dr = grad[:half], grad[half:]
    return p * (dp - jnp.sum(p * dp, axis=0, keepdims=True)) - r * (
        dr - jnp.sum(r * dr, axis=0, keepdims=True)
    )


def iota(shape, axis):
    return lax.broadcasted_iota(jnp.int32, shape, axis)


NEAR_FIRST = (1, 7, 2, 6, 3, 5, 4)
ROWS = 128
HALF = 64
TOKENS = ROWS * RING * RING
LINE = RING * HALF


def layer_kernel(
    q_ref, k_ref, v_ref, wq_ref, wk_ref,
    out_g, out_k, out_loss,
    kbuf, vbuf, scores, f_high, f_low, best, state, state_sum, total, accum,
    krow, vrow, e_row, kag, arows, acol,
    x, b1, t1, b2, suffix, g, g1, g1s, g2, g2s, tile, tiles, tile_x, l1, l1s, l2, gp, ba, bas, bb, bbs,
    kv_send, k_recv, v_recv, send, recv,
):
    z, y, xx = lax.axis_index(Z), lax.axis_index(Y), lax.axis_index(X)
    me = z * RING + y
    place = {Z: z, Y: y}
    others = [lax.rem(xx + d, 4) for d in (2, 1, 3)]
    near = [(axis, around(place[axis], d)) for axis in (Z, Y) for d in (1, -1)]
    greet(near + [(X, p) for p in others])

    k_streams = ((kbuf, kv_send.at[0], k_recv, 0, Y, Z), (kbuf, kv_send.at[1], k_recv, 1, Z, Y))
    v_streams = ((vbuf, kv_send.at[2], v_recv, 0, Y, Z), (vbuf, kv_send.at[3], v_recv, 1, Z, Y))

    def piece(stream, along, across):
        line = around(place[stream[5]], across)
        return (stream[3] * RING + line) * RING + around(place[stream[4]], along)

    def push(stream, src, at, axis, step):
        to = around(place[axis], step)
        remote(src, stream[0].at[at], stream[1], stream[2].at[at], axis, to).start()

    def forward(stream, at, axis, step):
        push(stream, stream[0].at[at], at, axis, step)

    def arrived(stream, at):
        block = stream[0].at[at]
        remote(block, block, stream[1], stream[2].at[at], Z, z).wait_recv()

    halves = (pl.ds(0, HALF), pl.ds(HALF, HALF))
    for stream in k_streams:
        at, src = piece(stream, 0, 0), k_ref.at[halves[stream[3]]]
        for axis in (stream[4], stream[5]):
            for way in (1, -1):
                push(stream, src, at, axis, way)
    for stream in v_streams:
        at, src = piece(stream, 0, 0), v_ref.at[halves[stream[3]]]
        for way in (1, -1):
            push(stream, src, at, stream[4], way)

    for ref, streams in ((k_ref, k_streams), (v_ref, v_streams)):
        for stream in streams:
            stream[0][piece(stream, 0, 0)] = ref[halves[stream[3]]]
    best[...] = jnp.full(best.shape, LOW, F32)
    for ref in (state, state_sum, total, accum):
        ref[...] = jnp.zeros_like(ref)
    queries = [q_ref[:, h, :] for h in range(2)]
    q_all = jnp.concatenate(queries, axis=0)
    wk = three(wk_ref[...].reshape(2 * HALF, 128))

    for hop in range(1, 5):
        for way in (1, -1):
            if hop == 4 and way == -1:
                continue
            for stream in k_streams + v_streams:
                at = piece(stream, -way * hop, 0)
                arrived(stream, at)
                if hop < (4 if way == 1 else 3):
                    forward(stream, at, stream[4], way)
                if stream[0] is kbuf:
                    forward(stream, at, stream[5], 1)
                    forward(stream, at, stream[5], -1)

    def pass_on(streams, hop):
        for along in (0, -1, 1, -2, 2, -3, 3, 4):
            for way in (1, -1):
                last = (way == 1) == (along % 2 == 0)
                if hop == 4 and not last:
                    continue
                for stream in streams:
                    at = piece(stream, along, -way * hop)
                    arrived(stream, at)
                    if hop < 3 or (hop == 3 and last):
                        forward(stream, at, stream[5], way)

    first = me * ROWS
    bound = first - WINDOW
    scale = 128 ** (-0.5)
    lane = iota((1, LINE), 1)
    lane_block, lane_row = jnp.right_shift(lane, 6), jnp.bitwise_and(lane, HALF - 1)
    query_place = first + jnp.bitwise_and(iota((2 * ROWS, 1), 0), ROWS - 1)

    def lanes(fold, start, value):
        for k in range(LINE // 128):
            start = fold(start, value[:, k * 128 : (k + 1) * 128])
        return start

    def on_keys(c):
        line = jnp.bitwise_and(c, RING - 1)
        second = c >= RING
        at = jnp.where(second, line * ROWS + HALF, line * (ROWS * RING))
        at = at + lane_block * jnp.where(second, ROWS * RING, ROWS) + lane_row
        kc = kbuf[pl.ds(c * RING, RING)].reshape(LINE, 128)
        s = dot(q_all, kc, NT) * scale
        s = jnp.where(at <= query_place, s, LOW)
        scores[c] = s
        best[...] = lanes(jnp.maximum, best[...], s)
        f = jnp.where(at < bound, features_of(wk, kc), 0.0)
        state_sum[...] = lanes(jnp.add, state_sum[...], f)
        f_high[c], f_low[c] = two(f)

    def on_values(top, c):
        vc = vbuf[pl.ds(c * RING, RING)].reshape(LINE, 128)
        w = jnp.exp(scores[c] - top)
        total[...] = lanes(jnp.add, total[...], w)
        accum[...] += dot(w.astype(BF16), vc)
        state[...] += dot(f_high[c], vc) + dot(f_low[c], vc)

    def lines(hop, work):
        @pl.loop(0, 4 if 0 < hop < 4 else 2)
        def _(i):
            second = jnp.bitwise_and(i, 1)
            steps = jnp.where(i < 2, RING - hop, RING + hop)
            c = second * RING + lax.rem(jnp.where(second == 1, y, z) + steps, RING)

            @pl.when(jnp.logical_or(second == 1, c <= z))
            def _():
                work(c)

    lines(0, on_keys)
    for hop in range(1, 5):
        pass_on(k_streams, hop)
        if hop == 3:
            for stream in v_streams:
                for along in (0, -1, 1, -2, 2, -3, 3, 4):
                    at = piece(stream, along, 0)
                    for way in (1, -1):
                        forward(stream, at, stream[5], way)
        lines(hop, on_keys)
    top = jnp.max(best[...], axis=1, keepdims=True)
    on_values = functools.partial(on_values, top)
    lines(0, on_values)

    before = jnp.where(y > 0, (RING + y - 1) * RING + z, (2 * RING - 1) * RING + jnp.maximum(z - 1, 0))
    tt, jj = iota((ROWS, 2 * ROWS), 0), iota((ROWS, 2 * ROWS), 1)
    window = (jj > tt) & (jj <= tt + WINDOW) & (bound + jj >= 0)
    tt, jj = iota((ROWS, ROWS), 0), iota((ROWS, ROWS), 1)
    linear_mask = (jj <= tt) & (bound + jj >= 0)
    turned_mask = (tt <= jj) & (bound + tt >= 0)
    kext = jnp.concatenate([kbuf[before], k_ref[...], k_ref[pl.ds(HALF, HALF)]], axis=0)
    kf_all = features_of(wk, kext[:ROWS])
    heads = []
    for h in range(2):
        q = queries[h]
        s = dot(q, kext, NT) * scale
        window_best = jnp.max(jnp.where(window, s, LOW), axis=1, keepdims=True)
        weights = jnp.where(window, jnp.exp(s - window_best), 0.0)
        window_total = jnp.sum(weights, axis=1, keepdims=True)
        qft = features_of(three(wq_ref[h]), q)
        qf = qft.T
        kft = kf_all[h * ROWS : (h + 1) * ROWS]
        linear = jnp.where(linear_mask, dot_wide(qf, kft), 0.0)
        prefix_sum = jnp.sum(state_sum[h * ROWS : (h + 1) * ROWS, :], axis=1, keepdims=True)
        linear_total = jnp.sum(linear, axis=1, keepdims=True) + dot_wide(
            qf, jnp.broadcast_to(prefix_sum, (128, 128))
        )
        lift = jnp.exp(-window_best)
        inverse = 1.0 / (window_total + lift * linear_total)
        heads.append((q, weights.astype(BF16), qft, qf, kft, linear, prefix_sum, lift, inverse))

    for hop in range(1, 5):
        pass_on(v_streams, hop)
        lines(hop, on_values)

    vext = jnp.concatenate([vbuf[before], v_ref[...], v_ref[pl.ds(HALF, HALF)]], axis=0)
    teacher = accum[...] / jnp.sum(total[...], axis=1, keepdims=True)
    teacher = teacher.astype(BF16).astype(F32)
    loss = jnp.zeros((8, 128), F32)
    kept = []
    for h in range(2):
        q, weights, qft, qf, kft, linear, prefix_sum, lift, inverse = heads[h]
        prefix = state[h * ROWS : (h + 1) * ROWS, :]
        window_sum = dot(weights, vext)
        linear_sum = dot_left(linear, vext[:ROWS]) + dot_wide(qf, prefix)
        student = (window_sum + lift * linear_sum) * inverse
        difference = student - teacher[h * ROWS : (h + 1) * ROWS]
        square = difference * difference
        for k in range(ROWS // 8):
            loss = loss + square[k * 8 : (k + 1) * 8]
        grad_out = difference * (2.0 / TOKENS)
        num_grad = lift * grad_out * inverse
        den_grad = -lift * jnp.sum(grad_out * student, axis=1, keepdims=True) * inverse
        dgt = den_grad.T
        adjoint = dot_wide(qft, num_grad)
        a_row = dot_wide(jnp.broadcast_to(dgt[:1], (8, ROWS)), qft, NT)
        for k in range(4):
            x[4 * h + k, 0:32] = adjoint[32 * k : 32 * (k + 1)]
            x[4 * h + k, 32:33] = a_row[:1]
        kept.append((prefix, num_grad, dgt))

    def start(k, axis, src, dst):
        for d in FAR_FIRST:
            p = around(place[axis], d)
            remote(src(p), dst.at[place[axis]], send.at[k], recv.at[k, place[axis]], axis, p).start()

    def finish(k, axis, dst):
        for d in NEAR_FIRST:
            p = around(place[axis], d)
            remote(dst.at[p], dst.at[p], send.at[k], recv.at[k, p], axis, p).wait_recv()

    def added(ref, low=0, high=RING):
        out = ref[low]
        for k in range(low + 1, high):
            out = out + ref[k]
        return out

    start(0, Y, lambda p: x.at[p], b1)
    b1[y] = x[y]
    tile[...] = loss
    for p in others:
        remote(tile, tiles.at[xx], send.at[1], recv.at[1, xx], X, p).start()
    tiles[xx] = loss

    for h in range(2):
        q, weights, qft, qf, kft, linear, prefix_sum, lift, inverse = heads[h]
        prefix, num_grad, dgt = kept[h]
        ngt = num_grad.T
        link = jnp.where(turned_mask, dot_right(vext[:ROWS], ngt) + dgt[:1], 0.0)
        qfg = dot_wide(kft, link) + dot_wide(prefix, ngt) + prefix_sum * dgt[:1]
        kfg = dot_wide(qft, link, NT)
        grad_query = dot_left(features_back(qft, qfg), q)
        grad_key = dot_left(features_back(kft, kfg), kext[:ROWS])
        for k in range(4):
            g[4 * h + k, 0:16] = grad_query[16 * k : 16 * (k + 1)]
            g[4 * h + k, 16:32] = grad_key[16 * k : 16 * (k + 1)]
    start(2, Z, lambda p: g.at[p], g1)
    g1[z] = g[z]

    own_head, part = jnp.right_shift(y, 2), jnp.bitwise_and(y, 3)
    sign = jnp.where(part < 2, 1.0, -1.0).astype(F32)
    within = pl.multiple_of(jnp.bitwise_and(part, 1) * 32, 32)
    for k in range(RING):
        if k:
            at = (RING + k - 1) * RING + z
        else:
            at = (2 * RING - 1) * RING + jnp.maximum(z - 1, 0)
        for row, buf in ((krow, kbuf), (vrow, vbuf)):
            row[k, 0:HALF] = buf[at]
            row[k, HALF:ROWS] = buf[z * RING + k]
    keys_row = krow[...].reshape(RING * ROWS, 128)
    pieces = three(wk_ref[own_head])
    act = dot(pieces[0], keys_row, NT) + (dot(pieces[1], keys_row, NT) + dot(pieces[2], keys_row, NT))
    e = jnp.exp(act * sign)
    e_row[...] = e * (1.0 / jnp.sum(e, axis=0, keepdims=True))

    finish(0, Y, b1)
    t1[...] = added(b1)
    start(3, Z, lambda p: t1, b2)
    for p in others:
        remote(tile, tiles.at[p], send.at[1], recv.at[1, p], X, p).wait_recv()
    tile_x[...] = added(tiles, 0, 4)
    start(4, Z, lambda p: tile_x, l1)
    l1[z] = tile_x[...]
    finish(2, Z, g1)
    g1s[...] = added(g1)
    start(5, Y, lambda p: g1s, g2)
    g2[y] = g1s[...]
    b2[z] = t1[...]
    finish(3, Z, b2)

    base = jnp.zeros((33, 128), F32)
    for k in range(1, RING):
        base = base + jnp.where(k > z, b2[k], 0.0)
    for k in reversed(range(RING)):
        suffix[k] = base
        arows[k : k + 1, :] = base[32:33]
        base = base + b1[k]
    acol[...] = arows[...].T
    columns = acol[pl.ds(pl.multiple_of(part * 32, 32), 32), :]
    grads = []
    for k in range(RING):
        grads.append(dot_left(suffix[k, 0:32], vrow[k], NT) + columns[:, k : k + 1])
    weighted = jnp.concatenate(grads, axis=1) * e_row[pl.ds(within, 32), :]
    kag[...] = -e_row[...] * jnp.sum(weighted, axis=0, keepdims=True)
    kag[pl.ds(within, 32), :] += weighted
    real = (iota((1, RING * ROWS), 1) >= HALF) | (z > 0)
    far = dot_left(jnp.where(real, kag[...] * sign, 0.0), keys_row)
    for k in range(RING):
        gp[k] = far[8 * k : 8 * (k + 1)]
    start(6, Z, lambda p: gp.at[p], ba)
    ba[z] = gp[z]

    finish(5, Y, g2)
    g2s[...] = added(g2)
    start(7, Z, lambda p: g2s, out_g)
    out_g[z] = g2s[...]
    finish(4, Z, l1)
    l1s[...] = added(l1)
    start(8, Y, lambda p: l1s, l2)
    l2[y] = l1s[...]

    finish(6, Z, ba)
    bas[...] = added(ba)
    start(9, Y, lambda p: bas, bb)
    bb[y] = bas[...]
    finish(9, Y, bb)
    bbs[0:8] = added(bb, 0, 4)
    bbs[8:16] = added(bb, 4, 8)
    start(10, Z, lambda p: bbs, out_k)
    out_k[z] = bbs[...]
    finish(8, Y, l2)
    out_loss[...] = added(l2)
    finish(7, Z, out_g)
    finish(10, Z, out_k)

    for stream in k_streams + v_streams:
        sent = stream[0].at[pl.ds(0, RING * RING - 1)]
        remote(sent, sent, stream[1], stream[2].at[0], Z, z).wait_send()
    for k, ref, count in (
        (0, b1, 7), (1, tiles, 3), (2, g1, 7), (3, b2, 7), (4, l1, 7), (5, g2, 7),
        (6, ba, 7), (7, out_g, 7), (8, l2, 7), (9, bb, 7), (10, out_k, 7),
    ):
        sent = ref.at[pl.ds(0, count)]
        remote(sent, sent, send.at[k], recv.at[k, 0], Z, z).wait_send()


VMEM = pl.BlockSpec(memory_space=pltpu.VMEM)


def layer(queries, keys, values, query_weight, key_weight):
    shape = jax.ShapeDtypeStruct
    dma = pltpu.SemaphoreType.DMA

    def f32(*dims):
        return pltpu.VMEM(dims, F32)

    def bf16(*dims):
        return pltpu.VMEM(dims, BF16)

    blocks = bf16(2 * RING * RING, HALF, 128)
    scratch = [
        blocks, blocks, f32(16, 256, LINE), bf16(16, 256, LINE), bf16(16, 256, LINE),
        f32(256, 128), f32(256, 128), f32(256, 128), f32(256, 128), f32(256, 128),
        bf16(8, 128, 128), bf16(8, 128, 128), f32(64, 1024), f32(64, 1024), f32(8, 128), f32(128, 8),
        f32(8, 33, 128), f32(8, 33, 128), f32(33, 128), f32(8, 33, 128), f32(8, 33, 128),
        f32(8, 32, 128), f32(8, 32, 128), f32(32, 128), f32(8, 32, 128), f32(32, 128),
        f32(8, 128), f32(4, 8, 128), f32(8, 128), f32(8, 8, 128), f32(8, 128), f32(8, 8, 128),
        f32(8, 8, 128), f32(8, 8, 128), f32(8, 128), f32(8, 8, 128), f32(16, 128),
        dma((4,)), dma((128,)), dma((128,)), dma((11,)), dma((11, RING)),
    ]
    return pl.pallas_call(
        layer_kernel,
        out_shape=(shape((8, 32, 128), F32), shape((8, 16, 128), F32), shape((8, 128), F32)),
        in_specs=[VMEM] * 5,
        out_specs=(VMEM,) * 3,
        scratch_shapes=scratch,
        compiler_params=pltpu.CompilerParams(
            collective_id=0, has_side_effects=True, vmem_limit_bytes=60 * 1024 * 1024
        ),
        name="layer",
    )(queries, keys, values, query_weight, key_weight)


def finish_kernel(g_ref, k_ref, loss_ref, loss, grad_query, grad_key):
    loss[0] = jnp.sum(loss_ref[...]) * (1.0 / TOKENS)
    grad_query[...] = g_ref[:, 0:16].reshape(2, HALF, 128)
    near = g_ref[:, 16:32].reshape(2, HALF, 128)
    for h in range(2):
        grad_key[h] = near[h] + k_ref[:, 8 * h : 8 * (h + 1)].reshape(HALF, 128)


def local(queries, keys, values, query_weight, key_weight):
    shape = jax.ShapeDtypeStruct
    return pl.pallas_call(
        finish_kernel,
        out_shape=(
            shape((1,), F32), shape(query_weight.shape, F32), shape(key_weight.shape, F32)
        ),
        in_specs=[VMEM] * 3,
        out_specs=(pl.BlockSpec(memory_space=pltpu.SMEM), VMEM, VMEM),
        name="finish",
    )(*layer(queries, keys, values, query_weight, key_weight))


def solution(mesh):
    split = Mesh(
        mesh.devices.reshape(8, 8, mesh.shape["head"], mesh.shape["rep"]),
        (Z, Y, X, "rep"),
    )
    return jax.shard_map(
        local,
        mesh=split,
        in_specs=(
            P(REP_SEQ, X, None),
            P(REP_SEQ, None),
            P(REP_SEQ, None),
            P(("rep", X), None, None),
            P(("rep", X), None, None),
        ),
        out_specs=(P("rep"), P(("rep", X), None, None), P(("rep", X), None, None)),
        check_vma=False,
    )
```

```python
import functools

import jax
import jax.numpy as jnp
from jax import lax
from jax.experimental import pallas as pl
from jax.experimental.pallas import tpu as pltpu
from jax.sharding import Mesh
from jax.sharding import PartitionSpec as P

WINDOW = 64
Z, Y, X = "seq_0", "seq_1", "head"
REP_SEQ = ("rep", Z, Y)
MESH = pl.DeviceIdType.MESH
RING = 8
LOW = -1e30
F32 = jnp.float32
BF16 = jnp.bfloat16
FAR_FIRST = (4, 3, 5, 2, 6, 1, 7)


def around(place, steps):
    return lax.rem(place + (steps + RING), RING)


def remote(src, dst, send, recv, axis, place):
    return pltpu.make_async_remote_copy(
        src_ref=src,
        dst_ref=dst,
        send_sem=send,
        recv_sem=recv,
        device_id={axis: place},
        device_id_type=MESH,
    )


def greet(peers):
    barrier = pltpu.get_barrier_semaphore()
    for axis, place in peers:
        pl.semaphore_signal(barrier, inc=1, device_id={axis: place}, device_id_type=MESH)
    pl.semaphore_wait(barrier, len(peers))


NN = (((1,), (0,)), ((), ()))
NT = (((1,), (1,)), ((), ()))


def dot(a, b, dims=NN):
    return lax.dot_general(a, b, dims, preferred_element_type=F32)


def two(a):
    high = a.astype(BF16)
    return high, (a - high.astype(F32)).astype(BF16)


def dot_wide(a, b, dims=NN):
    a_high, a_low = two(a)
    b_high, b_low = two(b)
    return dot(a_high, b_high, dims) + (dot(a_high, b_low, dims) + dot(a_low, b_high, dims))


def dot_left(a, b, dims=NN):
    high, low = two(a)
    return dot(high, b, dims) + dot(low, b, dims)


def dot_right(a, b, dims=NN):
    high, low = two(b)
    return dot(a, high, dims) + dot(a, low, dims)


def three(a):
    high = a.astype(BF16)
    rest = a - high.astype(F32)
    mid = rest.astype(BF16)
    return high, mid, (rest - mid.astype(F32)).astype(BF16)


def features_of(pieces, tokens):
    act = dot(pieces[0], tokens, NT) + (dot(pieces[1], tokens, NT) + dot(pieces[2], tokens, NT))
    half = 64
    parts = []
    for h in range(act.shape[0] // half):
        one = act[h * half : (h + 1) * half]
        for e in (jnp.exp(one), jnp.exp(-one)):
            parts.append(e * (1.0 / jnp.sum(e, axis=0, keepdims=True)))
    return jnp.concatenate(parts, axis=0)


def features_back(features, grad):
    half = features.shape[0] // 2
    p, r = features[:half], features[half:]
    dp, dr = grad[:half], grad[half:]
    return p * (dp - jnp.sum(p * dp, axis=0, keepdims=True)) - r * (
        dr - jnp.sum(r * dr, axis=0, keepdims=True)
    )


def iota(shape, axis):
    return lax.broadcasted_iota(jnp.int32, shape, axis)


NEAR_FIRST = (1, 7, 2, 6, 3, 5, 4)
ROWS = 128
HALF = 64
TOKENS = ROWS * RING * RING
LINE = RING * HALF


def layer_kernel(
    q_ref, k_ref, v_ref, wq_ref, wk_ref,
    out_g, out_k, out_loss,
    kbuf, vbuf, scores, f_high, f_low, best, state, state_sum, total, accum,
    krow, vrow, e_row, kag, arows, acol,
    x, b1, t1, b2, suffix, g, g1, g1s, g2, g2s, tile, tiles, tile_x, l1, l1s, l2, gp, ba, bas, bb, bbs,
    kv_send, k_recv, v_recv, send, recv,
):
    z, y, xx = lax.axis_index(Z), lax.axis_index(Y), lax.axis_index(X)
    me = z * RING + y
    place = {Z: z, Y: y}
    others = [lax.rem(xx + d, 4) for d in (2, 1, 3)]
    greet([(axis, around(place[axis], d)) for d in FAR_FIRST for axis in (Z, Y)] + [(X, p) for p in others])

    k_streams = ((kbuf, kv_send.at[0], k_recv, 0, Y, Z), (kbuf, kv_send.at[1], k_recv, 1, Z, Y))
    v_streams = ((vbuf, kv_send.at[2], v_recv, 0, Y, Z), (vbuf, kv_send.at[3], v_recv, 1, Z, Y))

    def piece(stream, along, across):
        line = around(place[stream[5]], across)
        return (stream[3] * RING + line) * RING + around(place[stream[4]], along)

    def push(stream, src, at, axis, step):
        to = around(place[axis], step)
        remote(src, stream[0].at[at], stream[1], stream[2].at[at], axis, to).start()

    def forward(stream, at, axis, step):
        push(stream, stream[0].at[at], at, axis, step)

    def arrived(stream, at):
        block = stream[0].at[at]
        remote(block, block, stream[1], stream[2].at[at], Z, z).wait_recv()

    halves = (pl.ds(0, HALF), pl.ds(HALF, HALF))
    for stream in k_streams:
        at, src = piece(stream, 0, 0), k_ref.at[halves[stream[3]]]
        for way in (1, -1):
            push(stream, src, at, stream[5], way)
    for ref, streams in ((k_ref, k_streams), (v_ref, v_streams)):
        for step in (1, 7, 4, 3, 5, 2, 6):
            for stream in streams:
                push(stream, ref.at[halves[stream[3]]], piece(stream, 0, 0), stream[4], step)
    for stream in v_streams:
        at, src = piece(stream, 0, 0), v_ref.at[halves[stream[3]]]
        for way in (1, -1):
            push(stream, src, at, stream[5], way)

    for ref, streams in ((k_ref, k_streams), (v_ref, v_streams)):
        for stream in streams:
            stream[0][piece(stream, 0, 0)] = ref[halves[stream[3]]]
    best[...] = jnp.full(best.shape, LOW, F32)
    for ref in (state, state_sum, total, accum):
        ref[...] = jnp.zeros_like(ref)
    queries = [q_ref[:, h, :] for h in range(2)]
    q_all = jnp.concatenate(queries, axis=0)
    wk = three(wk_ref[...].reshape(2 * HALF, 128))

    for streams in (k_streams, v_streams):
        for along in NEAR_FIRST:
            for stream in streams:
                at = piece(stream, along, 0)
                arrived(stream, at)
                forward(stream, at, stream[5], 1)
                forward(stream, at, stream[5], -1)

    def pass_on(streams, hop):
        for along in (0, -1, 1, -2, 2, -3, 3, 4):
            for way in (1, -1):
                last = (way == 1) == (along % 2 == 0)
                if hop == 4 and not last:
                    continue
                for stream in streams:
                    at = piece(stream, along, -way * hop)
                    arrived(stream, at)
                    if hop < 3 or (hop == 3 and last):
                        forward(stream, at, stream[5], way)

    first = me * ROWS
    bound = first - WINDOW
    scale = 128 ** (-0.5)
    lane = iota((1, LINE), 1)
    lane_block, lane_row = jnp.right_shift(lane, 6), jnp.bitwise_and(lane, HALF - 1)
    query_place = first + jnp.bitwise_and(iota((2 * ROWS, 1), 0), ROWS - 1)

    def lanes(fold, start, value):
        for k in range(LINE // 128):
            start = fold(start, value[:, k * 128 : (k + 1) * 128])
        return start

    def on_keys(c):
        line = jnp.bitwise_and(c, RING - 1)
        second = c >= RING
        at = jnp.where(second, line * ROWS + HALF, line * (ROWS * RING))
        at = at + lane_block * jnp.where(second, ROWS * RING, ROWS) + lane_row
        kc = kbuf[pl.ds(c * RING, RING)].reshape(LINE, 128)
        s = dot(q_all, kc, NT) * scale
        s = jnp.where(at <= query_place, s, LOW)
        scores[c] = s
        best[...] = lanes(jnp.maximum, best[...], s)
        f = jnp.where(at < bound, features_of(wk, kc), 0.0)
        state_sum[...] = lanes(jnp.add, state_sum[...], f)
        f_high[c], f_low[c] = two(f)

    def on_values(top, c):
        vc = vbuf[pl.ds(c * RING, RING)].reshape(LINE, 128)
        w = jnp.exp(scores[c] - top)
        total[...] = lanes(jnp.add, total[...], w)
        accum[...] += dot(w.astype(BF16), vc)
        state[...] += dot(f_high[c], vc) + dot(f_low[c], vc)

    def lines(hop, work):
        @pl.loop(0, 4 if 0 < hop < 4 else 2)
        def _(i):
            second = jnp.bitwise_and(i, 1)
            steps = jnp.where(i < 2, RING - hop, RING + hop)
            c = second * RING + lax.rem(jnp.where(second == 1, y, z) + steps, RING)

            @pl.when(jnp.logical_or(second == 1, c <= z))
            def _():
                work(c)

    lines(0, on_keys)
    for hop in range(1, 5):
        pass_on(k_streams, hop)
        lines(hop, on_keys)
        if hop < 4:
            pass_on(v_streams, hop)
    top = jnp.max(best[...], axis=1, keepdims=True)
    on_values = functools.partial(on_values, top)

    before = jnp.where(y > 0, (RING + y - 1) * RING + z, (2 * RING - 1) * RING + jnp.maximum(z - 1, 0))
    tt, jj = iota((ROWS, 2 * ROWS), 0), iota((ROWS, 2 * ROWS), 1)
    window = (jj > tt) & (jj <= tt + WINDOW) & (bound + jj >= 0)
    tt, jj = iota((ROWS, ROWS), 0), iota((ROWS, ROWS), 1)
    linear_mask = (jj <= tt) & (bound + jj >= 0)
    turned_mask = (tt <= jj) & (bound + tt >= 0)
    kext = jnp.concatenate([kbuf[before], k_ref[...], k_ref[pl.ds(HALF, HALF)]], axis=0)
    kf_all = features_of(wk, kext[:ROWS])
    heads = []
    for h in range(2):
        q = queries[h]
        s = dot(q, kext, NT) * scale
        window_best = jnp.max(jnp.where(window, s, LOW), axis=1, keepdims=True)
        weights = jnp.where(window, jnp.exp(s - window_best), 0.0)
        window_total = jnp.sum(weights, axis=1, keepdims=True)
        qft = features_of(three(wq_ref[h]), q)
        qf = qft.T
        kft = kf_all[h * ROWS : (h + 1) * ROWS]
        linear = jnp.where(linear_mask, dot_wide(qf, kft), 0.0)
        prefix_sum = jnp.sum(state_sum[h * ROWS : (h + 1) * ROWS, :], axis=1, keepdims=True)
        linear_total = jnp.sum(linear, axis=1, keepdims=True) + dot_wide(
            qf, jnp.broadcast_to(prefix_sum, (128, 128))
        )
        lift = jnp.exp(-window_best)
        inverse = 1.0 / (window_total + lift * linear_total)
        heads.append((q, weights.astype(BF16), qft, qf, kft, linear, prefix_sum, lift, inverse))

    for hop in range(4):
        lines(hop, on_values)
    pass_on(v_streams, 4)
    lines(4, on_values)

    vext = jnp.concatenate([vbuf[before], v_ref[...], v_ref[pl.ds(HALF, HALF)]], axis=0)
    teacher = accum[...] / jnp.sum(total[...], axis=1, keepdims=True)
    teacher = teacher.astype(BF16).astype(F32)
    loss = jnp.zeros((8, 128), F32)
    kept = []
    for h in range(2):
        q, weights, qft, qf, kft, linear, prefix_sum, lift, inverse = heads[h]
        prefix = state[h * ROWS : (h + 1) * ROWS, :]
        window_sum = dot(weights, vext)
        linear_sum = dot_left(linear, vext[:ROWS]) + dot_wide(qf, prefix)
        student = (window_sum + lift * linear_sum) * inverse
        difference = student - teacher[h * ROWS : (h + 1) * ROWS]
        square = difference * difference
        for k in range(ROWS // 8):
            loss = loss + square[k * 8 : (k + 1) * 8]
        grad_out = difference * (2.0 / TOKENS)
        num_grad = lift * grad_out * inverse
        den_grad = -lift * jnp.sum(grad_out * student, axis=1, keepdims=True) * inverse
        dgt = den_grad.T
        adjoint = dot_wide(qft, num_grad)
        a_row = dot_wide(jnp.broadcast_to(dgt[:1], (8, ROWS)), qft, NT)
        for k in range(4):
            x[4 * h + k, 0:32] = adjoint[32 * k : 32 * (k + 1)]
            x[4 * h + k, 32:33] = a_row[:1]
        kept.append((prefix, num_grad, dgt))

    def start(k, axis, src, dst):
        for d in FAR_FIRST:
            p = around(place[axis], d)
            remote(src(p), dst.at[place[axis]], send.at[k], recv.at[k, place[axis]], axis, p).start()

    def finish(k, axis, dst):
        for d in NEAR_FIRST:
            p = around(place[axis], d)
            remote(dst.at[p], dst.at[p], send.at[k], recv.at[k, p], axis, p).wait_recv()

    def added(ref, low=0, high=RING):
        out = ref[low]
        for k in range(low + 1, high):
            out = out + ref[k]
        return out

    start(0, Y, lambda p: x.at[p], b1)
    b1[y] = x[y]
    tile[...] = loss
    for p in others:
        remote(tile, tiles.at[xx], send.at[1], recv.at[1, xx], X, p).start()
    tiles[xx] = loss

    for h in range(2):
        q, weights, qft, qf, kft, linear, prefix_sum, lift, inverse = heads[h]
        prefix, num_grad, dgt = kept[h]
        ngt = num_grad.T
        link = jnp.where(turned_mask, dot_right(vext[:ROWS], ngt) + dgt[:1], 0.0)
        qfg = dot_wide(kft, link) + dot_wide(prefix, ngt) + prefix_sum * dgt[:1]
        kfg = dot_wide(qft, link, NT)
        grad_query = dot_left(features_back(qft, qfg), q)
        grad_key = dot_left(features_back(kft, kfg), kext[:ROWS])
        for k in range(4):
            g[4 * h + k, 0:16] = grad_query[16 * k : 16 * (k + 1)]
            g[4 * h + k, 16:32] = grad_key[16 * k : 16 * (k + 1)]
    start(2, Z, lambda p: g.at[p], g1)
    g1[z] = g[z]

    own_head, part = jnp.right_shift(y, 2), jnp.bitwise_and(y, 3)
    sign = jnp.where(part < 2, 1.0, -1.0).astype(F32)
    within = pl.multiple_of(jnp.bitwise_and(part, 1) * 32, 32)
    for k in range(RING):
        if k:
            at = (RING + k - 1) * RING + z
        else:
            at = (2 * RING - 1) * RING + jnp.maximum(z - 1, 0)
        for row, buf in ((krow, kbuf), (vrow, vbuf)):
            row[k, 0:HALF] = buf[at]
            row[k, HALF:ROWS] = buf[z * RING + k]
    keys_row = krow[...].reshape(RING * ROWS, 128)
    pieces = three(wk_ref[own_head])
    act = dot(pieces[0], keys_row, NT) + (dot(pieces[1], keys_row, NT) + dot(pieces[2], keys_row, NT))
    e = jnp.exp(act * sign)
    e_row[...] = e * (1.0 / jnp.sum(e, axis=0, keepdims=True))

    finish(0, Y, b1)
    t1[...] = added(b1)
    start(3, Z, lambda p: t1, b2)
    for p in others:
        remote(tile, tiles.at[p], send.at[1], recv.at[1, p], X, p).wait_recv()
    tile_x[...] = added(tiles, 0, 4)
    start(4, Z, lambda p: tile_x, l1)
    l1[z] = tile_x[...]
    finish(2, Z, g1)
    g1s[...] = added(g1)
    start(5, Y, lambda p: g1s, g2)
    g2[y] = g1s[...]
    b2[z] = t1[...]
    finish(3, Z, b2)

    base = jnp.zeros((33, 128), F32)
    for k in range(1, RING):
        base = base + jnp.where(k > z, b2[k], 0.0)
    for k in reversed(range(RING)):
        suffix[k] = base
        arows[k : k + 1, :] = base[32:33]
        base = base + b1[k]
    acol[...] = arows[...].T
    columns = acol[pl.ds(pl.multiple_of(part * 32, 32), 32), :]
    grads = []
    for k in range(RING):
        grads.append(dot_left(suffix[k, 0:32], vrow[k], NT) + columns[:, k : k + 1])
    weighted = jnp.concatenate(grads, axis=1) * e_row[pl.ds(within, 32), :]
    kag[...] = -e_row[...] * jnp.sum(weighted, axis=0, keepdims=True)
    kag[pl.ds(within, 32), :] += weighted
    real = (iota((1, RING * ROWS), 1) >= HALF) | (z > 0)
    far = dot_left(jnp.where(real, kag[...] * sign, 0.0), keys_row)
    for k in range(RING):
        gp[k] = far[8 * k : 8 * (k + 1)]
    start(6, Z, lambda p: gp.at[p], ba)
    ba[z] = gp[z]

    finish(5, Y, g2)
    g2s[...] = added(g2)
    start(7, Z, lambda p: g2s, out_g)
    out_g[z] = g2s[...]
    finish(4, Z, l1)
    l1s[...] = added(l1)
    start(8, Y, lambda p: l1s, l2)
    l2[y] = l1s[...]

    finish(6, Z, ba)
    bas[...] = added(ba)
    start(9, Y, lambda p: bas, bb)
    bb[y] = bas[...]
    finish(9, Y, bb)
    bbs[0:8] = added(bb, 0, 4)
    bbs[8:16] = added(bb, 4, 8)
    start(10, Z, lambda p: bbs, out_k)
    out_k[z] = bbs[...]
    finish(8, Y, l2)
    out_loss[...] = added(l2)
    finish(7, Z, out_g)
    finish(10, Z, out_k)

    for stream in k_streams + v_streams:
        sent = stream[0].at[pl.ds(0, RING * RING - 1)]
        remote(sent, sent, stream[1], stream[2].at[0], Z, z).wait_send()
    for k, ref, count in (
        (0, b1, 7), (1, tiles, 3), (2, g1, 7), (3, b2, 7), (4, l1, 7), (5, g2, 7),
        (6, ba, 7), (7, out_g, 7), (8, l2, 7), (9, bb, 7), (10, out_k, 7),
    ):
        sent = ref.at[pl.ds(0, count)]
        remote(sent, sent, send.at[k], recv.at[k, 0], Z, z).wait_send()


VMEM = pl.BlockSpec(memory_space=pltpu.VMEM)


def layer(queries, keys, values, query_weight, key_weight):
    shape = jax.ShapeDtypeStruct
    dma = pltpu.SemaphoreType.DMA

    def f32(*dims):
        return pltpu.VMEM(dims, F32)

    def bf16(*dims):
        return pltpu.VMEM(dims, BF16)

    blocks = bf16(2 * RING * RING, HALF, 128)
    scratch = [
        blocks, blocks, f32(16, 256, LINE), bf16(16, 256, LINE), bf16(16, 256, LINE),
        f32(256, 128), f32(256, 128), f32(256, 128), f32(256, 128), f32(256, 128),
        bf16(8, 128, 128), bf16(8, 128, 128), f32(64, 1024), f32(64, 1024), f32(8, 128), f32(128, 8),
        f32(8, 33, 128), f32(8, 33, 128), f32(33, 128), f32(8, 33, 128), f32(8, 33, 128),
        f32(8, 32, 128), f32(8, 32, 128), f32(32, 128), f32(8, 32, 128), f32(32, 128),
        f32(8, 128), f32(4, 8, 128), f32(8, 128), f32(8, 8, 128), f32(8, 128), f32(8, 8, 128),
        f32(8, 8, 128), f32(8, 8, 128), f32(8, 128), f32(8, 8, 128), f32(16, 128),
        dma((4,)), dma((128,)), dma((128,)), dma((11,)), dma((11, RING)),
    ]
    return pl.pallas_call(
        layer_kernel,
        out_shape=(shape((8, 32, 128), F32), shape((8, 16, 128), F32), shape((8, 128), F32)),
        in_specs=[VMEM] * 5,
        out_specs=(VMEM,) * 3,
        scratch_shapes=scratch,
        compiler_params=pltpu.CompilerParams(
            collective_id=0, has_side_effects=True, vmem_limit_bytes=60 * 1024 * 1024
        ),
        name="layer",
    )(queries, keys, values, query_weight, key_weight)


def finish_kernel(g_ref, k_ref, loss_ref, loss, grad_query, grad_key):
    loss[0] = jnp.sum(loss_ref[...]) * (1.0 / TOKENS)
    grad_query[...] = g_ref[:, 0:16].reshape(2, HALF, 128)
    near = g_ref[:, 16:32].reshape(2, HALF, 128)
    for h in range(2):
        grad_key[h] = near[h] + k_ref[:, 8 * h : 8 * (h + 1)].reshape(HALF, 128)


def local(queries, keys, values, query_weight, key_weight):
    shape = jax.ShapeDtypeStruct
    return pl.pallas_call(
        finish_kernel,
        out_shape=(
            shape((1,), F32), shape(query_weight.shape, F32), shape(key_weight.shape, F32)
        ),
        in_specs=[VMEM] * 3,
        out_specs=(pl.BlockSpec(memory_space=pltpu.SMEM), VMEM, VMEM),
        name="finish",
    )(*layer(queries, keys, values, query_weight, key_weight))


def solution(mesh):
    split = Mesh(
        mesh.devices.reshape(8, 8, mesh.shape["head"], mesh.shape["rep"]),
        (Z, Y, X, "rep"),
    )
    return jax.shard_map(
        local,
        mesh=split,
        in_specs=(
            P(REP_SEQ, X, None),
            P(REP_SEQ, None),
            P(REP_SEQ, None),
            P(("rep", X), None, None),
            P(("rep", X), None, None),
        ),
        out_specs=(P("rep"), P(("rep", X), None, None), P(("rep", X), None, None)),
        check_vma=False,
    )
```

```python
import functools

import jax
import jax.numpy as jnp
from jax import lax
from jax.experimental import pallas as pl
from jax.experimental.pallas import tpu as pltpu
from jax.sharding import Mesh
from jax.sharding import PartitionSpec as P

WINDOW = 64
Z, Y, X = "seq_0", "seq_1", "head"
REP_SEQ = ("rep", Z, Y)
MESH = pl.DeviceIdType.MESH
RING = 8
LOW = -1e30
F32 = jnp.float32
BF16 = jnp.bfloat16
FAR_FIRST = (4, 3, 5, 2, 6, 1, 7)


def around(place, steps):
    return lax.rem(place + (steps + RING), RING)


def remote(src, dst, send, recv, axis, place):
    return pltpu.make_async_remote_copy(
        src_ref=src,
        dst_ref=dst,
        send_sem=send,
        recv_sem=recv,
        device_id={axis: place},
        device_id_type=MESH,
    )


def greet(peers):
    barrier = pltpu.get_barrier_semaphore()
    for axis, place in peers:
        pl.semaphore_signal(barrier, inc=1, device_id={axis: place}, device_id_type=MESH)
    pl.semaphore_wait(barrier, len(peers))


NN = (((1,), (0,)), ((), ()))
NT = (((1,), (1,)), ((), ()))


def dot(a, b, dims=NN):
    return lax.dot_general(a, b, dims, preferred_element_type=F32)


def two(a):
    high = a.astype(BF16)
    return high, (a - high.astype(F32)).astype(BF16)


def dot_wide(a, b, dims=NN):
    a_high, a_low = two(a)
    b_high, b_low = two(b)
    return dot(a_high, b_high, dims) + (dot(a_high, b_low, dims) + dot(a_low, b_high, dims))


def dot_left(a, b, dims=NN):
    high, low = two(a)
    return dot(high, b, dims) + dot(low, b, dims)


def dot_right(a, b, dims=NN):
    high, low = two(b)
    return dot(a, high, dims) + dot(a, low, dims)


def three(a):
    high = a.astype(BF16)
    rest = a - high.astype(F32)
    mid = rest.astype(BF16)
    return high, mid, (rest - mid.astype(F32)).astype(BF16)


def features_of(pieces, tokens):
    act = dot(pieces[0], tokens, NT) + (dot(pieces[1], tokens, NT) + dot(pieces[2], tokens, NT))
    half = 64
    parts = []
    for h in range(act.shape[0] // half):
        one = act[h * half : (h + 1) * half]
        for e in (jnp.exp(one), jnp.exp(-one)):
            parts.append(e * (1.0 / jnp.sum(e, axis=0, keepdims=True)))
    return jnp.concatenate(parts, axis=0)


def features_back(features, grad):
    half = features.shape[0] // 2
    p, r = features[:half], features[half:]
    dp, dr = grad[:half], grad[half:]
    return p * (dp - jnp.sum(p * dp, axis=0, keepdims=True)) - r * (
        dr - jnp.sum(r * dr, axis=0, keepdims=True)
    )


def iota(shape, axis):
    return lax.broadcasted_iota(jnp.int32, shape, axis)


NEAR_FIRST = (1, 7, 2, 6, 3, 5, 4)
ROWS = 128
HALF = 64
TOKENS = ROWS * RING * RING
LINE = RING * HALF


def layer_kernel(
    q_ref, k_ref, v_ref, wq_ref, wk_ref,
    out_g, out_k, out_loss,
    kbuf, vbuf, scores, f_high, f_low, best, state, state_sum, total, accum,
    far, g, g1, g1s, g2, g2s, tile, tiles, tile_x, l1, l1s, l2, gk, k1, k1s, k2, k2s,
    kv_send, k_recv, v_recv, send, recv,
):
    z, y, xx = lax.axis_index(Z), lax.axis_index(Y), lax.axis_index(X)
    me = z * RING + y
    place = {Z: z, Y: y}
    others = [lax.rem(xx + d, 4) for d in (2, 1, 3)]
    greet([(axis, around(place[axis], d)) for d in FAR_FIRST for axis in (Z, Y)] + [(X, p) for p in others])

    k_streams = ((kbuf, kv_send.at[0], k_recv, 0, Y, Z), (kbuf, kv_send.at[1], k_recv, 1, Z, Y))
    v_streams = ((vbuf, kv_send.at[2], v_recv, 0, Y, Z), (vbuf, kv_send.at[3], v_recv, 1, Z, Y))

    def piece(stream, along, across):
        line = around(place[stream[5]], across)
        return (stream[3] * RING + line) * RING + around(place[stream[4]], along)

    def push(stream, src, at, axis, step):
        to = around(place[axis], step)
        remote(src, stream[0].at[at], stream[1], stream[2].at[at], axis, to).start()

    def forward(stream, at, axis, step):
        push(stream, stream[0].at[at], at, axis, step)

    def arrived(stream, at):
        block = stream[0].at[at]
        remote(block, block, stream[1], stream[2].at[at], Z, z).wait_recv()

    halves = (pl.ds(0, HALF), pl.ds(HALF, HALF))
    for stream in k_streams:
        at, src = piece(stream, 0, 0), k_ref.at[halves[stream[3]]]
        for way in (1, -1):
            push(stream, src, at, stream[5], way)
    for ref, streams in ((k_ref, k_streams), (v_ref, v_streams)):
        for step in (1, 7, 4, 3, 5, 2, 6):
            for stream in streams:
                push(stream, ref.at[halves[stream[3]]], piece(stream, 0, 0), stream[4], step)
    for stream in v_streams:
        at, src = piece(stream, 0, 0), v_ref.at[halves[stream[3]]]
        for way in (1, -1):
            push(stream, src, at, stream[5], way)

    for ref, streams in ((k_ref, k_streams), (v_ref, v_streams)):
        for stream in streams:
            stream[0][piece(stream, 0, 0)] = ref[halves[stream[3]]]
    best[...] = jnp.full(best.shape, LOW, F32)
    for ref in (state, state_sum, total, accum):
        ref[...] = jnp.zeros_like(ref)
    queries = [q_ref[:, h, :] for h in range(2)]
    q_all = jnp.concatenate(queries, axis=0)
    wk = three(wk_ref[...].reshape(2 * HALF, 128))

    for streams in (k_streams, v_streams):
        for along in NEAR_FIRST:
            for stream in streams:
                at = piece(stream, along, 0)
                arrived(stream, at)
                forward(stream, at, stream[5], 1)
                forward(stream, at, stream[5], -1)

    def pass_on(streams, hop):
        for along in (0, -1, 1, -2, 2, -3, 3, 4):
            for way in (1, -1):
                last = (way == 1) == (along % 2 == 0)
                if hop == 4 and not last:
                    continue
                for stream in streams:
                    at = piece(stream, along, -way * hop)
                    arrived(stream, at)
                    if hop < 3 or (hop == 3 and last):
                        forward(stream, at, stream[5], way)

    first = me * ROWS
    bound = first - WINDOW
    scale = 128 ** (-0.5)
    lane = iota((1, LINE), 1)
    lane_block, lane_row = jnp.right_shift(lane, 6), jnp.bitwise_and(lane, HALF - 1)
    query_place = first + jnp.bitwise_and(iota((2 * ROWS, 1), 0), ROWS - 1)

    def lanes(fold, start, value):
        for k in range(LINE // 128):
            start = fold(start, value[:, k * 128 : (k + 1) * 128])
        return start

    def on_keys(c):
        line = jnp.bitwise_and(c, RING - 1)
        second = c >= RING
        at = jnp.where(second, line * ROWS + HALF, line * (ROWS * RING))
        at = at + lane_block * jnp.where(second, ROWS * RING, ROWS) + lane_row
        kc = kbuf[pl.ds(c * RING, RING)].reshape(LINE, 128)
        s = dot(q_all, kc, NT) * scale
        s = jnp.where(at <= query_place, s, LOW)
        scores[c] = s
        best[...] = lanes(jnp.maximum, best[...], s)
        f = jnp.where(at < bound, features_of(wk, kc), 0.0)
        state_sum[...] = lanes(jnp.add, state_sum[...], f)
        f_high[c], f_low[c] = two(f)

    def on_state(c):
        vc = vbuf[pl.ds(c * RING, RING)].reshape(LINE, 128)
        state[...] += dot(f_high[c], vc) + dot(f_low[c], vc)

    def on_weights(top, c):
        vc = vbuf[pl.ds(c * RING, RING)].reshape(LINE, 128)
        w = jnp.exp(scores[c] - top)
        total[...] = lanes(jnp.add, total[...], w)
        accum[...] += dot(w.astype(BF16), vc)

    def on_grads(adjoint, a_column, c):
        kc = kbuf[pl.ds(c * RING, RING)].reshape(LINE, 128)
        vc = vbuf[pl.ds(c * RING, RING)].reshape(LINE, 128)
        grad = dot(adjoint[0], vc, NT) + dot(adjoint[1], vc, NT) + a_column
        f = f_high[c].astype(F32) + f_low[c].astype(F32)
        back = [features_back(f[i : i + ROWS], grad[i : i + ROWS]) for i in (0, ROWS)]
        far[...] += dot_left(jnp.concatenate(back, axis=0), kc)

    def lines(hop, work):
        @pl.loop(0, 4 if 0 < hop < 4 else 2)
        def _(i):
            second = jnp.bitwise_and(i, 1)
            steps = jnp.where(i < 2, RING - hop, RING + hop)
            c = second * RING + lax.rem(jnp.where(second == 1, y, z) + steps, RING)

            @pl.when(jnp.logical_or(second == 1, c <= z))
            def _():
                work(c)

    before = jnp.where(y > 0, (RING + y - 1) * RING + z, (2 * RING - 1) * RING + jnp.maximum(z - 1, 0))
    tt, jj = iota((ROWS, 2 * ROWS), 0), iota((ROWS, 2 * ROWS), 1)
    window = (jj > tt) & (jj <= tt + WINDOW) & (bound + jj >= 0)
    tt, jj = iota((ROWS, ROWS), 0), iota((ROWS, ROWS), 1)
    linear_mask = (jj <= tt) & (bound + jj >= 0)
    turned_mask = (tt <= jj) & (bound + tt >= 0)

    def nearby(h):
        kext = jnp.concatenate([kbuf[before], k_ref[...], k_ref[pl.ds(HALF, HALF)]], axis=0)
        q = queries[h]
        s = dot(q, kext, NT) * scale
        window_best = jnp.max(jnp.where(window, s, LOW), axis=1, keepdims=True)
        weights = jnp.where(window, jnp.exp(s - window_best), 0.0)
        window_total = jnp.sum(weights, axis=1, keepdims=True)
        qft = features_of(three(wq_ref[h]), q)
        qf = qft.T
        kft = features_of([w[h * HALF : (h + 1) * HALF] for w in wk], kext[:ROWS])
        linear = jnp.where(linear_mask, dot_wide(qf, kft), 0.0)
        linear_total = jnp.sum(linear, axis=1, keepdims=True)
        lift = jnp.exp(-window_best)
        return q, weights.astype(BF16), window_total, qft, qf, kft, linear, linear_total, lift

    heads = []
    lines(0, on_keys)
    lines(0, on_state)
    for hop in range(1, 5):
        pass_on(k_streams, hop)
        lines(hop, on_keys)
        if hop < 4:
            pass_on(v_streams, hop)
            lines(hop, on_state)
        if 0 < hop < 3:
            heads.append(nearby(hop - 1))
    top = jnp.max(best[...], axis=1, keepdims=True)
    for hop in range(4):
        lines(hop, functools.partial(on_weights, top))
    pass_on(v_streams, 4)
    lines(4, on_state)
    lines(4, functools.partial(on_weights, top))

    kext = jnp.concatenate([kbuf[before], k_ref[pl.ds(0, HALF)]], axis=0)
    vext = jnp.concatenate([vbuf[before], v_ref[...], v_ref[pl.ds(HALF, HALF)]], axis=0)
    teacher = accum[...] / jnp.sum(total[...], axis=1, keepdims=True)
    teacher = teacher.astype(BF16).astype(F32)
    loss = jnp.zeros((8, 128), F32)
    kept, adjoint, a_column = [], [], []
    for h in range(2):
        q, weights, window_total, qft, qf, kft, linear, linear_total, lift = heads[h]
        prefix = state[h * ROWS : (h + 1) * ROWS, :]
        prefix_sum = jnp.sum(state_sum[h * ROWS : (h + 1) * ROWS, :], axis=1, keepdims=True)
        linear_total = linear_total + dot_wide(qf, jnp.broadcast_to(prefix_sum, (128, 128)))
        inverse = 1.0 / (window_total + lift * linear_total)
        window_sum = dot(weights, vext)
        linear_sum = dot_left(linear, vext[:ROWS]) + dot_wide(qf, prefix)
        student = (window_sum + lift * linear_sum) * inverse
        difference = student - teacher[h * ROWS : (h + 1) * ROWS]
        square = difference * difference
        for k in range(ROWS // 8):
            loss = loss + square[k * 8 : (k + 1) * 8]
        grad_out = difference * (2.0 / TOKENS)
        num_grad = lift * grad_out * inverse
        den_grad = -lift * jnp.sum(grad_out * student, axis=1, keepdims=True) * inverse
        dgt = den_grad.T
        adjoint.append(dot_wide(qft, num_grad))
        a_column.append(jnp.sum(qft * dgt[:1], axis=1, keepdims=True))
        kept.append((prefix, prefix_sum, num_grad, dgt))
    tile[...] = loss
    for p in others:
        remote(tile, tiles.at[xx], send.at[3], recv.at[3, xx], X, p).start()
    tiles[xx] = loss

    def start(k, axis, src, dst):
        for d in FAR_FIRST:
            p = around(place[axis], d)
            remote(src(p), dst.at[place[axis]], send.at[k], recv.at[k, place[axis]], axis, p).start()

    def finish(k, axis, dst):
        for d in NEAR_FIRST:
            p = around(place[axis], d)
            remote(dst.at[p], dst.at[p], send.at[k], recv.at[k, p], axis, p).wait_recv()

    def added(ref, low=0, high=RING):
        out = ref[low]
        for k in range(low + 1, high):
            out = out + ref[k]
        return out

    near = []
    for h in range(2):
        q, weights, window_total, qft, qf, kft = heads[h][:6]
        prefix, prefix_sum, num_grad, dgt = kept[h]
        ngt = num_grad.T
        link = jnp.where(turned_mask, dot_right(vext[:ROWS], ngt) + dgt[:1], 0.0)
        qfg = dot_wide(kft, link) + dot_wide(prefix, ngt) + prefix_sum * dgt[:1]
        kfg = dot_wide(qft, link, NT)
        grad_query = dot_left(features_back(qft, qfg), q)
        for k in range(4):
            g[4 * h + k] = grad_query[16 * k : 16 * (k + 1)]
        near.append(dot_left(features_back(kft, kfg), kext))
    start(0, Z, lambda p: g.at[p], g1)
    g1[z] = g[z]

    far[...] = jnp.concatenate(near, axis=0)
    work = functools.partial(
        on_grads, two(jnp.concatenate(adjoint, axis=0)), jnp.concatenate(a_column, axis=0)
    )
    for hop in range(5):
        lines(hop, work)
    for h in range(2):
        for k in range(RING):
            gk[h, k] = far[h * HALF + 8 * k : h * HALF + 8 * (k + 1)]

    ways = ((Y, Z, y, z), (Z, Y, z, y))
    for h, (one, other, mine, across) in enumerate(ways):
        start(6 + h, one, lambda p, h=h: gk.at[h, p], k1.at[h])
        k1[h, mine] = gk[h, mine]
    for p in others:
        remote(tile, tiles.at[p], send.at[3], recv.at[3, p], X, p).wait_recv()
    tile_x[...] = added(tiles, 0, 4)
    start(4, Z, lambda p: tile_x, l1)
    l1[z] = tile_x[...]
    finish(0, Z, g1)
    g1s[...] = added(g1)
    start(1, Y, lambda p: g1s, g2)
    g2[y] = g1s[...]
    for h, (one, other, mine, across) in enumerate(ways):
        finish(6 + h, one, k1.at[h])
        k1s[h] = added(k1[h])
        start(8 + h, other, lambda p, h=h: k1s.at[h], k2.at[h])
        k2[h, across] = k1s[h]
    finish(4, Z, l1)
    l1s[...] = added(l1)
    start(5, Y, lambda p: l1s, l2)
    l2[y] = l1s[...]
    finish(1, Y, g2)
    g2s[...] = added(g2)
    start(2, Z, lambda p: g2s, out_g)
    out_g[z] = g2s[...]
    for h, (one, other, mine, across) in enumerate(ways):
        finish(8 + h, other, k2.at[h])
        k2s[h] = added(k2[h])
        start(10 + h, one, lambda p, h=h: k2s.at[h], out_k.at[h])
        out_k[h, mine] = k2s[h]
    finish(5, Y, l2)
    out_loss[...] = added(l2)
    finish(2, Z, out_g)
    for h, (one, other, mine, across) in enumerate(ways):
        finish(10 + h, one, out_k.at[h])

    for stream in k_streams + v_streams:
        sent = stream[0].at[pl.ds(0, RING * RING - 1)]
        remote(sent, sent, stream[1], stream[2].at[0], Z, z).wait_send()
    for k, ref, count in (
        (0, g1, 7), (1, g2, 7), (2, out_g, 7), (3, tiles, 3), (4, l1, 7), (5, l2, 7),
        (6, k1.at[0], 7), (7, k1.at[1], 7), (8, k2.at[0], 7), (9, k2.at[1], 7),
        (10, out_k.at[0], 7), (11, out_k.at[1], 7),
    ):
        sent = ref.at[pl.ds(0, count)]
        remote(sent, sent, send.at[k], recv.at[k, 0], Z, z).wait_send()


VMEM = pl.BlockSpec(memory_space=pltpu.VMEM)


def layer(queries, keys, values, query_weight, key_weight):
    shape = jax.ShapeDtypeStruct
    dma = pltpu.SemaphoreType.DMA

    def f32(*dims):
        return pltpu.VMEM(dims, F32)

    def bf16(*dims):
        return pltpu.VMEM(dims, BF16)

    blocks = bf16(2 * RING * RING, HALF, 128)
    scratch = [
        blocks, blocks, f32(16, 256, LINE), bf16(16, 256, LINE), bf16(16, 256, LINE),
        f32(256, 128), f32(256, 128), f32(256, 128), f32(256, 128), f32(256, 128),
        f32(128, 128), f32(8, 16, 128), f32(8, 16, 128), f32(16, 128), f32(8, 16, 128), f32(16, 128),
        f32(8, 128), f32(4, 8, 128), f32(8, 128), f32(8, 8, 128), f32(8, 128), f32(8, 8, 128),
        f32(2, 8, 8, 128), f32(2, 8, 8, 128), f32(2, 8, 128), f32(2, 8, 8, 128), f32(2, 8, 128),
        dma((4,)), dma((128,)), dma((128,)), dma((12,)), dma((12, RING)),
    ]
    return pl.pallas_call(
        layer_kernel,
        out_shape=(shape((8, 16, 128), F32), shape((2, 8, 8, 128), F32), shape((8, 128), F32)),
        in_specs=[VMEM] * 5,
        out_specs=(VMEM,) * 3,
        scratch_shapes=scratch,
        compiler_params=pltpu.CompilerParams(
            collective_id=0, has_side_effects=True, vmem_limit_bytes=60 * 1024 * 1024
        ),
        name="layer",
    )(queries, keys, values, query_weight, key_weight)


def finish_kernel(g_ref, k_ref, loss_ref, loss, grad_query, grad_key):
    loss[0] = jnp.sum(loss_ref[...]) * (1.0 / TOKENS)
    grad_query[...] = g_ref[...].reshape(2, HALF, 128)
    grad_key[...] = k_ref[...].reshape(2, HALF, 128)


def local(queries, keys, values, query_weight, key_weight):
    shape = jax.ShapeDtypeStruct
    return pl.pallas_call(
        finish_kernel,
        out_shape=(
            shape((1,), F32), shape(query_weight.shape, F32), shape(key_weight.shape, F32)
        ),
        in_specs=[VMEM] * 3,
        out_specs=(pl.BlockSpec(memory_space=pltpu.SMEM), VMEM, VMEM),
        name="finish",
    )(*layer(queries, keys, values, query_weight, key_weight))


def solution(mesh):
    split = Mesh(
        mesh.devices.reshape(8, 8, mesh.shape["head"], mesh.shape["rep"]),
        (Z, Y, X, "rep"),
    )
    return jax.shard_map(
        local,
        mesh=split,
        in_specs=(
            P(REP_SEQ, X, None),
            P(REP_SEQ, None),
            P(REP_SEQ, None),
            P(("rep", X), None, None),
            P(("rep", X), None, None),
        ),
        out_specs=(P("rep"), P(("rep", X), None, None), P(("rep", X), None, None)),
        check_vma=False,
    )
```

```python
import functools

import jax
import jax.numpy as jnp
from jax import lax
from jax.experimental import pallas as pl
from jax.experimental.pallas import tpu as pltpu
from jax.sharding import Mesh
from jax.sharding import PartitionSpec as P

WINDOW = 64
Z, Y, X = "seq_0", "seq_1", "head"
REP_SEQ = ("rep", Z, Y)
MESH = pl.DeviceIdType.MESH
RING = 8
LOW = -1e30
F32 = jnp.float32
BF16 = jnp.bfloat16
FAR_FIRST = (4, 3, 5, 2, 6, 1, 7)


def around(place, steps):
    return lax.rem(place + (steps + RING), RING)


def remote(src, dst, send, recv, axis, place):
    return pltpu.make_async_remote_copy(
        src_ref=src,
        dst_ref=dst,
        send_sem=send,
        recv_sem=recv,
        device_id={axis: place},
        device_id_type=MESH,
    )


def greet(peers):
    barrier = pltpu.get_barrier_semaphore()
    for axis, place in peers:
        pl.semaphore_signal(barrier, inc=1, device_id={axis: place}, device_id_type=MESH)
    pl.semaphore_wait(barrier, len(peers))


NN = (((1,), (0,)), ((), ()))
NT = (((1,), (1,)), ((), ()))


def dot(a, b, dims=NN):
    return lax.dot_general(a, b, dims, preferred_element_type=F32)


def two(a):
    high = a.astype(BF16)
    return high, (a - high.astype(F32)).astype(BF16)


def dot_wide(a, b, dims=NN):
    a_high, a_low = two(a)
    b_high, b_low = two(b)
    return dot(a_high, b_high, dims) + (dot(a_high, b_low, dims) + dot(a_low, b_high, dims))


def dot_left(a, b, dims=NN):
    high, low = two(a)
    return dot(high, b, dims) + dot(low, b, dims)


def dot_right(a, b, dims=NN):
    high, low = two(b)
    return dot(a, high, dims) + dot(a, low, dims)


def three(a):
    high = a.astype(BF16)
    rest = a - high.astype(F32)
    mid = rest.astype(BF16)
    return high, mid, (rest - mid.astype(F32)).astype(BF16)


def features_of(pieces, tokens):
    act = dot(pieces[0], tokens, NT) + (dot(pieces[1], tokens, NT) + dot(pieces[2], tokens, NT))
    half = 64
    parts = []
    for h in range(act.shape[0] // half):
        one = act[h * half : (h + 1) * half]
        for e in (jnp.exp(one), jnp.exp(-one)):
            parts.append(e * (1.0 / jnp.sum(e, axis=0, keepdims=True)))
    return jnp.concatenate(parts, axis=0)


def features_back(features, grad):
    half = features.shape[0] // 2
    p, r = features[:half], features[half:]
    dp, dr = grad[:half], grad[half:]
    return p * (dp - jnp.sum(p * dp, axis=0, keepdims=True)) - r * (
        dr - jnp.sum(r * dr, axis=0, keepdims=True)
    )


def iota(shape, axis):
    return lax.broadcasted_iota(jnp.int32, shape, axis)


NEAR_FIRST = (1, 7, 2, 6, 3, 5, 4)
ROWS = 128
HALF = 64
TOKENS = ROWS * RING * RING
LINE = RING * HALF


def layer_kernel(
    q_ref, k_ref, v_ref, wq_ref, wk_ref,
    out_g, out_k, out_loss,
    kbuf, vbuf, scores, f_high, f_low, best, state, state_sum, total, accum,
    far, g, g1, g1s, g2, g2s, tile, tiles, tile_x, l1, l1s, l2, gk, k1, k1s, k2, k2s,
    kv_send, k_recv, v_recv, send, recv,
):
    z, y, xx = lax.axis_index(Z), lax.axis_index(Y), lax.axis_index(X)
    me = z * RING + y
    place = {Z: z, Y: y}
    others = [lax.rem(xx + d, 4) for d in (2, 1, 3)]
    greet([(axis, around(place[axis], d)) for d in FAR_FIRST for axis in (Z, Y)] + [(X, p) for p in others])

    k_streams = ((kbuf, kv_send.at[0], k_recv, 0, Y, Z), (kbuf, kv_send.at[1], k_recv, 1, Z, Y))
    v_streams = ((vbuf, kv_send.at[2], v_recv, 0, Y, Z), (vbuf, kv_send.at[3], v_recv, 1, Z, Y))

    def piece(stream, along, across):
        line = around(place[stream[5]], across)
        return (stream[3] * RING + line) * RING + around(place[stream[4]], along)

    def push(stream, src, at, axis, step):
        to = around(place[axis], step)
        remote(src, stream[0].at[at], stream[1], stream[2].at[at], axis, to).start()

    def forward(stream, at, axis, step):
        push(stream, stream[0].at[at], at, axis, step)

    def arrived(stream, at):
        block = stream[0].at[at]
        remote(block, block, stream[1], stream[2].at[at], Z, z).wait_recv()

    halves = (pl.ds(0, HALF), pl.ds(HALF, HALF))
    for stream in k_streams:
        at, src = piece(stream, 0, 0), k_ref.at[halves[stream[3]]]
        for way in (1, -1):
            push(stream, src, at, stream[5], way)
    for ref, streams in ((k_ref, k_streams), (v_ref, v_streams)):
        for step in (1, 7, 4, 3, 5, 2, 6):
            for stream in streams:
                push(stream, ref.at[halves[stream[3]]], piece(stream, 0, 0), stream[4], step)
    for stream in v_streams:
        at, src = piece(stream, 0, 0), v_ref.at[halves[stream[3]]]
        for way in (1, -1):
            push(stream, src, at, stream[5], way)

    for ref, streams in ((k_ref, k_streams), (v_ref, v_streams)):
        for stream in streams:
            stream[0][piece(stream, 0, 0)] = ref[halves[stream[3]]]
    best[...] = jnp.full(best.shape, LOW, F32)
    for ref in (state, state_sum, total, accum):
        ref[...] = jnp.zeros_like(ref)
    queries = [q_ref[:, h, :] for h in range(2)]
    q_all = jnp.concatenate(queries, axis=0)
    wk = three(wk_ref[...].reshape(2 * HALF, 128))

    for streams in (k_streams, v_streams):
        for along in NEAR_FIRST:
            for stream in streams:
                at = piece(stream, along, 0)
                arrived(stream, at)
                forward(stream, at, stream[5], 1)
                forward(stream, at, stream[5], -1)

    def pass_on(streams, hop):
        for along in (0, -1, 1, -2, 2, -3, 3, 4):
            for way in (1, -1):
                last = (way == 1) == (along % 2 == 0)
                if hop == 4 and not last:
                    continue
                for stream in streams:
                    at = piece(stream, along, -way * hop)
                    arrived(stream, at)
                    if hop < 3 or (hop == 3 and last):
                        forward(stream, at, stream[5], way)

    first = me * ROWS
    bound = first - WINDOW
    scale = 128 ** (-0.5)
    lane = iota((1, LINE), 1)
    lane_block, lane_row = jnp.right_shift(lane, 6), jnp.bitwise_and(lane, HALF - 1)
    query_place = first + jnp.bitwise_and(iota((2 * ROWS, 1), 0), ROWS - 1)

    def lanes(fold, start, value):
        for k in range(LINE // 128):
            start = fold(start, value[:, k * 128 : (k + 1) * 128])
        return start

    def chunk(buf, c):
        return buf[pl.ds(c * RING, RING)].reshape(LINE, 128)

    def on_keys(cs):
        top, sums = best[...], state_sum[...]
        for c in cs:
            line = jnp.bitwise_and(c, RING - 1)
            second = c >= RING
            at = jnp.where(second, line * ROWS + HALF, line * (ROWS * RING))
            at = at + lane_block * jnp.where(second, ROWS * RING, ROWS) + lane_row
            kc = chunk(kbuf, c)
            s = dot(q_all, kc, NT) * scale
            s = jnp.where(at <= query_place, s, LOW)
            scores[c] = s
            top = lanes(jnp.maximum, top, s)
            f = jnp.where(at < bound, features_of(wk, kc), 0.0)
            sums = lanes(jnp.add, sums, f)
            f_high[c], f_low[c] = two(f)
        best[...], state_sum[...] = top, sums

    def on_state(cs):
        add = state[...]
        for c in cs:
            vc = chunk(vbuf, c)
            add = add + (dot(f_high[c], vc) + dot(f_low[c], vc))
        state[...] = add

    def on_weights(top, cs):
        sums, add = total[...], accum[...]
        for c in cs:
            w = jnp.exp(scores[c] - top)
            sums = lanes(jnp.add, sums, w)
            add = add + dot(w.astype(BF16), chunk(vbuf, c))
        total[...], accum[...] = sums, add

    def on_grads(adjoint, a_column, cs):
        add = far[...]
        for c in cs:
            vc = chunk(vbuf, c)
            grad = dot(adjoint[0], vc, NT) + dot(adjoint[1], vc, NT) + a_column
            f = f_high[c].astype(F32) + f_low[c].astype(F32)
            back = [features_back(f[i : i + ROWS], grad[i : i + ROWS]) for i in (0, ROWS)]
            add = add + dot_left(jnp.concatenate(back, axis=0), chunk(kbuf, c))
        far[...] = add

    def lines(hop, work):
        ways = (hop,) if hop in (0, 4) else (-hop, hop)
        work([c for way in ways for c in (around(z, way), RING + around(y, way))])

    before = jnp.where(y > 0, (RING + y - 1) * RING + z, (2 * RING - 1) * RING + jnp.maximum(z - 1, 0))
    tt, jj = iota((ROWS, 2 * ROWS), 0), iota((ROWS, 2 * ROWS), 1)
    window = (jj > tt) & (jj <= tt + WINDOW) & (bound + jj >= 0)
    tt, jj = iota((ROWS, ROWS), 0), iota((ROWS, ROWS), 1)
    linear_mask = (jj <= tt) & (bound + jj >= 0)
    turned_mask = (tt <= jj) & (bound + tt >= 0)

    def nearby(h):
        kext = jnp.concatenate([kbuf[before], k_ref[...], k_ref[pl.ds(HALF, HALF)]], axis=0)
        q = queries[h]
        s = dot(q, kext, NT) * scale
        window_best = jnp.max(jnp.where(window, s, LOW), axis=1, keepdims=True)
        weights = jnp.where(window, jnp.exp(s - window_best), 0.0)
        window_total = jnp.sum(weights, axis=1, keepdims=True)
        qft = features_of(three(wq_ref[h]), q)
        qf = qft.T
        kft = features_of([w[h * HALF : (h + 1) * HALF] for w in wk], kext[:ROWS])
        linear = jnp.where(linear_mask, dot_wide(qf, kft), 0.0)
        linear_total = jnp.sum(linear, axis=1, keepdims=True)
        lift = jnp.exp(-window_best)
        return q, weights.astype(BF16), window_total, qft, qf, kft, linear, linear_total, lift

    heads = []
    lines(0, on_keys)
    lines(0, on_state)
    for hop in range(1, 5):
        pass_on(k_streams, hop)
        lines(hop, on_keys)
        if hop < 4:
            pass_on(v_streams, hop)
            lines(hop, on_state)
        if 0 < hop < 3:
            heads.append(nearby(hop - 1))
    top = jnp.max(best[...], axis=1, keepdims=True)
    for hop in range(4):
        lines(hop, functools.partial(on_weights, top))
    pass_on(v_streams, 4)
    lines(4, on_state)
    lines(4, functools.partial(on_weights, top))

    kext = jnp.concatenate([kbuf[before], k_ref[pl.ds(0, HALF)]], axis=0)
    vext = jnp.concatenate([vbuf[before], v_ref[...], v_ref[pl.ds(HALF, HALF)]], axis=0)
    teacher = accum[...] / jnp.sum(total[...], axis=1, keepdims=True)
    teacher = teacher.astype(BF16).astype(F32)
    loss = jnp.zeros((8, 128), F32)
    kept, adjoint, a_column = [], [], []
    for h in range(2):
        q, weights, window_total, qft, qf, kft, linear, linear_total, lift = heads[h]
        prefix = state[h * ROWS : (h + 1) * ROWS, :]
        prefix_sum = jnp.sum(state_sum[h * ROWS : (h + 1) * ROWS, :], axis=1, keepdims=True)
        linear_total = linear_total + dot_wide(qf, jnp.broadcast_to(prefix_sum, (128, 128)))
        inverse = 1.0 / (window_total + lift * linear_total)
        window_sum = dot(weights, vext)
        linear_sum = dot_left(linear, vext[:ROWS]) + dot_wide(qf, prefix)
        student = (window_sum + lift * linear_sum) * inverse
        difference = student - teacher[h * ROWS : (h + 1) * ROWS]
        square = difference * difference
        for k in range(ROWS // 8):
            loss = loss + square[k * 8 : (k + 1) * 8]
        grad_out = difference * (2.0 / TOKENS)
        num_grad = lift * grad_out * inverse
        den_grad = -lift * jnp.sum(grad_out * student, axis=1, keepdims=True) * inverse
        dgt = den_grad.T
        adjoint.append(dot_wide(qft, num_grad))
        a_column.append(jnp.sum(qft * dgt[:1], axis=1, keepdims=True))
        kept.append((prefix, prefix_sum, num_grad, dgt))
    tile[...] = loss
    for p in others:
        remote(tile, tiles.at[xx], send.at[3], recv.at[3, xx], X, p).start()
    tiles[xx] = loss

    def start(k, axis, src, dst):
        for d in FAR_FIRST:
            p = around(place[axis], d)
            remote(src(p), dst.at[place[axis]], send.at[k], recv.at[k, place[axis]], axis, p).start()

    def finish(k, axis, dst):
        for d in NEAR_FIRST:
            p = around(place[axis], d)
            remote(dst.at[p], dst.at[p], send.at[k], recv.at[k, p], axis, p).wait_recv()

    def added(ref, low=0, high=RING):
        out = ref[low]
        for k in range(low + 1, high):
            out = out + ref[k]
        return out

    near = []
    for h in range(2):
        q, weights, window_total, qft, qf, kft = heads[h][:6]
        prefix, prefix_sum, num_grad, dgt = kept[h]
        ngt = num_grad.T
        link = jnp.where(turned_mask, dot_right(vext[:ROWS], ngt) + dgt[:1], 0.0)
        qfg = dot_wide(kft, link) + dot_wide(prefix, ngt) + prefix_sum * dgt[:1]
        kfg = dot_wide(qft, link, NT)
        grad_query = dot_left(features_back(qft, qfg), q)
        for k in range(4):
            g[4 * h + k] = grad_query[16 * k : 16 * (k + 1)]
        near.append(dot_left(features_back(kft, kfg), kext))
    start(0, Z, lambda p: g.at[p], g1)
    g1[z] = g[z]

    far[...] = jnp.concatenate(near, axis=0)
    work = functools.partial(
        on_grads, two(jnp.concatenate(adjoint, axis=0)), jnp.concatenate(a_column, axis=0)
    )
    for hop in range(5):
        lines(hop, work)
    for h in range(2):
        for k in range(RING):
            gk[h, k] = far[h * HALF + 8 * k : h * HALF + 8 * (k + 1)]

    ways = ((Y, Z, y, z), (Z, Y, z, y))
    for h, (one, other, mine, across) in enumerate(ways):
        start(6 + h, one, lambda p, h=h: gk.at[h, p], k1.at[h])
        k1[h, mine] = gk[h, mine]
    for p in others:
        remote(tile, tiles.at[p], send.at[3], recv.at[3, p], X, p).wait_recv()
    tile_x[...] = added(tiles, 0, 4)
    start(4, Z, lambda p: tile_x, l1)
    l1[z] = tile_x[...]
    finish(0, Z, g1)
    g1s[...] = added(g1)
    start(1, Y, lambda p: g1s, g2)
    g2[y] = g1s[...]
    for h, (one, other, mine, across) in enumerate(ways):
        finish(6 + h, one, k1.at[h])
        k1s[h] = added(k1[h])
        start(8 + h, other, lambda p, h=h: k1s.at[h], k2.at[h])
        k2[h, across] = k1s[h]
    finish(4, Z, l1)
    l1s[...] = added(l1)
    start(5, Y, lambda p: l1s, l2)
    l2[y] = l1s[...]
    finish(1, Y, g2)
    g2s[...] = added(g2)
    start(2, Z, lambda p: g2s, out_g)
    out_g[z] = g2s[...]
    for h, (one, other, mine, across) in enumerate(ways):
        finish(8 + h, other, k2.at[h])
        k2s[h] = added(k2[h])
        start(10 + h, one, lambda p, h=h: k2s.at[h], out_k.at[h])
        out_k[h, mine] = k2s[h]
    finish(5, Y, l2)
    out_loss[...] = added(l2)
    finish(2, Z, out_g)
    for h, (one, other, mine, across) in enumerate(ways):
        finish(10 + h, one, out_k.at[h])

    for stream in k_streams + v_streams:
        sent = stream[0].at[pl.ds(0, RING * RING - 1)]
        remote(sent, sent, stream[1], stream[2].at[0], Z, z).wait_send()
    for k, ref, count in (
        (0, g1, 7), (1, g2, 7), (2, out_g, 7), (3, tiles, 3), (4, l1, 7), (5, l2, 7),
        (6, k1.at[0], 7), (7, k1.at[1], 7), (8, k2.at[0], 7), (9, k2.at[1], 7),
        (10, out_k.at[0], 7), (11, out_k.at[1], 7),
    ):
        sent = ref.at[pl.ds(0, count)]
        remote(sent, sent, send.at[k], recv.at[k, 0], Z, z).wait_send()


VMEM = pl.BlockSpec(memory_space=pltpu.VMEM)


def layer(queries, keys, values, query_weight, key_weight):
    shape = jax.ShapeDtypeStruct
    dma = pltpu.SemaphoreType.DMA

    def f32(*dims):
        return pltpu.VMEM(dims, F32)

    def bf16(*dims):
        return pltpu.VMEM(dims, BF16)

    blocks = bf16(2 * RING * RING, HALF, 128)
    scratch = [
        blocks, blocks, f32(16, 256, LINE), bf16(16, 256, LINE), bf16(16, 256, LINE),
        f32(256, 128), f32(256, 128), f32(256, 128), f32(256, 128), f32(256, 128),
        f32(128, 128), f32(8, 16, 128), f32(8, 16, 128), f32(16, 128), f32(8, 16, 128), f32(16, 128),
        f32(8, 128), f32(4, 8, 128), f32(8, 128), f32(8, 8, 128), f32(8, 128), f32(8, 8, 128),
        f32(2, 8, 8, 128), f32(2, 8, 8, 128), f32(2, 8, 128), f32(2, 8, 8, 128), f32(2, 8, 128),
        dma((4,)), dma((128,)), dma((128,)), dma((12,)), dma((12, RING)),
    ]
    return pl.pallas_call(
        layer_kernel,
        out_shape=(shape((8, 16, 128), F32), shape((2, 8, 8, 128), F32), shape((8, 128), F32)),
        in_specs=[VMEM] * 5,
        out_specs=(VMEM,) * 3,
        scratch_shapes=scratch,
        compiler_params=pltpu.CompilerParams(
            collective_id=0, has_side_effects=True, vmem_limit_bytes=60 * 1024 * 1024
        ),
        name="layer",
    )(queries, keys, values, query_weight, key_weight)


def finish_kernel(g_ref, k_ref, loss_ref, loss, grad_query, grad_key):
    loss[0] = jnp.sum(loss_ref[...]) * (1.0 / TOKENS)
    grad_query[...] = g_ref[...].reshape(2, HALF, 128)
    grad_key[...] = k_ref[...].reshape(2, HALF, 128)


def local(queries, keys, values, query_weight, key_weight):
    shape = jax.ShapeDtypeStruct
    return pl.pallas_call(
        finish_kernel,
        out_shape=(
            shape((1,), F32), shape(query_weight.shape, F32), shape(key_weight.shape, F32)
        ),
        in_specs=[VMEM] * 3,
        out_specs=(pl.BlockSpec(memory_space=pltpu.SMEM), VMEM, VMEM),
        name="finish",
    )(*layer(queries, keys, values, query_weight, key_weight))


def solution(mesh):
    split = Mesh(
        mesh.devices.reshape(8, 8, mesh.shape["head"], mesh.shape["rep"]),
        (Z, Y, X, "rep"),
    )
    return jax.shard_map(
        local,
        mesh=split,
        in_specs=(
            P(REP_SEQ, X, None),
            P(REP_SEQ, None),
            P(REP_SEQ, None),
            P(("rep", X), None, None),
            P(("rep", X), None, None),
        ),
        out_specs=(P("rep"), P(("rep", X), None, None), P(("rep", X), None, None)),
        check_vma=False,
    )
```

```python
import functools

import jax
import jax.numpy as jnp
from jax import lax
from jax.experimental import pallas as pl
from jax.experimental.pallas import tpu as pltpu
from jax.sharding import Mesh
from jax.sharding import PartitionSpec as P

WINDOW = 64
Z, Y, X = "seq_0", "seq_1", "head"
REP_SEQ = ("rep", Z, Y)
MESH = pl.DeviceIdType.MESH
RING = 8
LOW = -1e30
F32 = jnp.float32
BF16 = jnp.bfloat16
FAR_FIRST = (4, 3, 5, 2, 6, 1, 7)


def around(place, steps):
    return lax.rem(place + (steps + RING), RING)


def remote(src, dst, send, recv, axis, place):
    return pltpu.make_async_remote_copy(
        src_ref=src,
        dst_ref=dst,
        send_sem=send,
        recv_sem=recv,
        device_id={axis: place},
        device_id_type=MESH,
    )


def greet(peers):
    barrier = pltpu.get_barrier_semaphore()
    for axis, place in peers:
        pl.semaphore_signal(barrier, inc=1, device_id={axis: place}, device_id_type=MESH)
    pl.semaphore_wait(barrier, len(peers))


NN = (((1,), (0,)), ((), ()))
NT = (((1,), (1,)), ((), ()))


def dot(a, b, dims=NN):
    return lax.dot_general(a, b, dims, preferred_element_type=F32)


def two(a):
    high = a.astype(BF16)
    return high, (a - high.astype(F32)).astype(BF16)


def dot_wide(a, b, dims=NN):
    a_high, a_low = two(a)
    b_high, b_low = two(b)
    return dot(a_high, b_high, dims) + (dot(a_high, b_low, dims) + dot(a_low, b_high, dims))


def dot_left(a, b, dims=NN):
    high, low = two(a)
    return dot(high, b, dims) + dot(low, b, dims)


def dot_right(a, b, dims=NN):
    high, low = two(b)
    return dot(a, high, dims) + dot(a, low, dims)


def three(a):
    high = a.astype(BF16)
    rest = a - high.astype(F32)
    mid = rest.astype(BF16)
    return high, mid, (rest - mid.astype(F32)).astype(BF16)


def features_of(pieces, tokens):
    act = sum(dot(piece, tokens, NT) for piece in pieces[1:]) + dot(pieces[0], tokens, NT)
    half = 64
    parts = []
    for h in range(act.shape[0] // half):
        one = act[h * half : (h + 1) * half]
        for e in (jnp.exp(one), jnp.exp(-one)):
            parts.append(e * (1.0 / jnp.sum(e, axis=0, keepdims=True)))
    return jnp.concatenate(parts, axis=0)


def features_back(features, grad):
    half = features.shape[0] // 2
    p, r = features[:half], features[half:]
    dp, dr = grad[:half], grad[half:]
    return p * (dp - jnp.sum(p * dp, axis=0, keepdims=True)) - r * (
        dr - jnp.sum(r * dr, axis=0, keepdims=True)
    )


def iota(shape, axis):
    return lax.broadcasted_iota(jnp.int32, shape, axis)


NEAR_FIRST = (1, 7, 2, 6, 3, 5, 4)
ROWS = 128
HALF = 64
TOKENS = ROWS * RING * RING
LINE = RING * HALF


def layer_kernel(
    q_ref, k_ref, v_ref, wq_ref, wk_ref,
    out_g, out_k, out_loss,
    kbuf, vbuf, scores, f_high, f_low, best, state, state_sum, total, accum,
    far, g, g1, g1s, g2, g2s, tile, tiles, tile_x, l1, l1s, l2, gk, k1, k1s, k2, k2s,
    kv_send, k_recv, v_recv, send, recv,
):
    z, y, xx = lax.axis_index(Z), lax.axis_index(Y), lax.axis_index(X)
    me = z * RING + y
    place = {Z: z, Y: y}
    others = [lax.rem(xx + d, 4) for d in (2, 1, 3)]
    close = [(axis, around(place[axis], d)) for d in (2, -2, 1, -1) for axis in (Z, Y)]
    greet(close + [(X, p) for p in others])

    k_streams = ((kbuf, kv_send.at[0], k_recv, 0, Y, Z), (kbuf, kv_send.at[1], k_recv, 1, Z, Y))
    v_streams = ((vbuf, kv_send.at[2], v_recv, 0, Y, Z), (vbuf, kv_send.at[3], v_recv, 1, Z, Y))

    def piece(stream, along, across):
        line = around(place[stream[5]], across)
        return (stream[3] * RING + line) * RING + around(place[stream[4]], along)

    def push(stream, src, at, axis, step):
        to = around(place[axis], step)
        remote(src, stream[0].at[at], stream[1], stream[2].at[at], axis, to).start()

    def forward(stream, at, axis, step):
        push(stream, stream[0].at[at], at, axis, step)

    def arrived(stream, at):
        block = stream[0].at[at]
        remote(block, block, stream[1], stream[2].at[at], Z, z).wait_recv()

    halves = (pl.ds(0, HALF), pl.ds(HALF, HALF))
    for stream in k_streams:
        at, src = piece(stream, 0, 0), k_ref.at[halves[stream[3]]]
        for way in (1, -1):
            push(stream, src, at, stream[5], way)
    for ref, streams in ((k_ref, k_streams), (v_ref, v_streams)):
        for step in (1, -1, 2, -2):
            for stream in streams:
                push(stream, ref.at[halves[stream[3]]], piece(stream, 0, 0), stream[4], step)
    for stream in v_streams:
        at, src = piece(stream, 0, 0), v_ref.at[halves[stream[3]]]
        for way in (1, -1):
            push(stream, src, at, stream[5], way)

    for ref, streams in ((k_ref, k_streams), (v_ref, v_streams)):
        for stream in streams:
            stream[0][piece(stream, 0, 0)] = ref[halves[stream[3]]]
    best[...] = jnp.full(best.shape, LOW, F32)
    for ref in (state, state_sum, total, accum):
        ref[...] = jnp.zeros_like(ref)
    queries = [q_ref[:, h, :] for h in range(2)]
    q_all = jnp.concatenate(queries, axis=0)
    wk = three(wk_ref[...].reshape(2 * HALF, 128))

    query_features = []
    for h in range(2):
        qft = features_of(three(wq_ref[h]), queries[h])
        query_features.append((qft, qft.T))

    for offsets in ((-1, 1, -2, 2), (-3, 3, 4)):
        for streams in (k_streams, v_streams):
            for along in offsets:
                for stream in streams:
                    at = piece(stream, along, 0)
                    arrived(stream, at)
                    if along == -2:
                        forward(stream, at, stream[4], 1)
                        if streams is k_streams:
                            forward(stream, at, stream[4], 2)
                    if along == 2:
                        forward(stream, at, stream[4], -1)
                        if streams is v_streams:
                            forward(stream, at, stream[4], -2)
                    forward(stream, at, stream[5], 1)
                    forward(stream, at, stream[5], -1)

    def pass_on(streams, hop):
        for along in (0, -1, 1, -2, 2, -3, 3, 4):
            for way in (1, -1):
                last = (way == 1) == (along % 2 == 0)
                if hop == 4 and not last:
                    continue
                for stream in streams:
                    at = piece(stream, along, -way * hop)
                    arrived(stream, at)
                    if hop < 3 or (hop == 3 and last):
                        forward(stream, at, stream[5], way)

    first = me * ROWS
    bound = first - WINDOW
    scale = 128 ** (-0.5)
    lane = iota((1, LINE), 1)
    lane_block, lane_row = jnp.right_shift(lane, 6), jnp.bitwise_and(lane, HALF - 1)
    query_place = first + jnp.bitwise_and(iota((2 * ROWS, 1), 0), ROWS - 1)

    def lanes(fold, start, value):
        for k in range(LINE // 128):
            start = fold(start, value[:, k * 128 : (k + 1) * 128])
        return start

    def chunk(buf, c):
        return buf[pl.ds(c * RING, RING)].reshape(LINE, 128)

    def on_keys(cs):
        top, sums = best[...], state_sum[...]
        for c in cs:
            line = jnp.bitwise_and(c, RING - 1)
            second = c >= RING
            at = jnp.where(second, line * ROWS + HALF, line * (ROWS * RING))
            at = at + lane_block * jnp.where(second, ROWS * RING, ROWS) + lane_row
            kc = chunk(kbuf, c)
            s = dot(q_all, kc, NT) * scale
            s = jnp.where(at <= query_place, s, LOW)
            scores[c] = s
            top = lanes(jnp.maximum, top, s)
            f = jnp.where(at < bound, features_of(wk[:2], kc), 0.0)
            sums = lanes(jnp.add, sums, f)
            f_high[c], f_low[c] = two(f)
        best[...], state_sum[...] = top, sums

    def on_state(cs):
        add = state[...]
        for c in cs:
            vc = chunk(vbuf, c)
            add = add + (dot(f_high[c], vc) + dot(f_low[c], vc))
        state[...] = add

    def on_weights(top, cs):
        sums, add = total[...], accum[...]
        for c in cs:
            w = jnp.exp(scores[c] - top)
            sums = lanes(jnp.add, sums, w)
            add = add + dot(w.astype(BF16), chunk(vbuf, c))
        total[...], accum[...] = sums, add

    def on_grads(adjoint, a_column, cs):
        add = far[...]
        for c in cs:
            vc = chunk(vbuf, c)
            grad = dot(adjoint[0], vc, NT) + dot(adjoint[1], vc, NT) + a_column
            f = f_high[c].astype(F32) + f_low[c].astype(F32)
            back = [features_back(f[i : i + ROWS], grad[i : i + ROWS]) for i in (0, ROWS)]
            add = add + dot_left(jnp.concatenate(back, axis=0), chunk(kbuf, c))
        far[...] = add

    def lines(hop, work):
        ways = (hop,) if hop in (0, 4) else (-hop, hop)
        work([c for way in ways for c in (around(z, way), RING + around(y, way))])

    before = jnp.where(y > 0, (RING + y - 1) * RING + z, (2 * RING - 1) * RING + jnp.maximum(z - 1, 0))
    tt, jj = iota((ROWS, 2 * ROWS), 0), iota((ROWS, 2 * ROWS), 1)
    window = (jj > tt) & (jj <= tt + WINDOW) & (bound + jj >= 0)
    tt, jj = iota((ROWS, ROWS), 0), iota((ROWS, ROWS), 1)
    linear_mask = (jj <= tt) & (bound + jj >= 0)
    turned_mask = (tt <= jj) & (bound + tt >= 0)

    def nearby(h):
        kext = jnp.concatenate([kbuf[before], k_ref[...], k_ref[pl.ds(HALF, HALF)]], axis=0)
        q = queries[h]
        s = dot(q, kext, NT) * scale
        window_best = jnp.max(jnp.where(window, s, LOW), axis=1, keepdims=True)
        weights = jnp.where(window, jnp.exp(s - window_best), 0.0)
        window_total = jnp.sum(weights, axis=1, keepdims=True)
        qft, qf = query_features[h]
        kft = features_of([w[h * HALF : (h + 1) * HALF] for w in wk], kext[:ROWS])
        linear = jnp.where(linear_mask, dot_wide(qf, kft), 0.0)
        linear_total = jnp.sum(linear, axis=1, keepdims=True)
        lift = jnp.exp(-window_best)
        return q, weights.astype(BF16), window_total, qft, qf, kft, linear, linear_total, lift

    def ready(h, head):
        q, weights, window_total, qft, qf, kft, linear, linear_total, lift = head
        vext = jnp.concatenate([vbuf[before], v_ref[...], v_ref[pl.ds(HALF, HALF)]], axis=0)
        prefix_sum = jnp.sum(state_sum[h * ROWS : (h + 1) * ROWS, :], axis=1, keepdims=True)
        linear_total = linear_total + dot_wide(qf, jnp.broadcast_to(prefix_sum, (128, 128)))
        inverse = 1.0 / (window_total + lift * linear_total)
        return q, qft, qf, kft, prefix_sum, lift, inverse, dot(weights, vext), dot_left(linear, vext[:ROWS])

    heads = []
    lines(0, on_keys)
    lines(0, on_state)
    for hop in (1, 2, 3):
        pass_on(k_streams, hop)
        lines(hop, on_keys)
        pass_on(v_streams, hop)
        lines(hop, on_state)
        if hop < 3:
            heads.append(nearby(hop - 1))
    pass_on(k_streams, 4)
    lines(4, on_keys)
    top = jnp.max(best[...], axis=1, keepdims=True)
    on_weights = functools.partial(on_weights, top)
    for hop in range(4):
        lines(hop, on_weights)
    heads = [ready(h, heads[h]) for h in range(2)]
    pass_on(v_streams, 4)
    lines(4, on_state)
    lines(4, on_weights)

    kext = jnp.concatenate([kbuf[before], k_ref[pl.ds(0, HALF)]], axis=0)
    vext = jnp.concatenate([vbuf[before], v_ref[pl.ds(0, HALF)]], axis=0)
    teacher = accum[...] / jnp.sum(total[...], axis=1, keepdims=True)
    teacher = teacher.astype(BF16).astype(F32)
    loss = jnp.zeros((8, 128), F32)
    kept, adjoint, a_column = [], [], []
    for h in range(2):
        q, qft, qf, kft, prefix_sum, lift, inverse, window_sum, linear_sum = heads[h]
        prefix = state[h * ROWS : (h + 1) * ROWS, :]
        linear_sum = linear_sum + dot_wide(qf, prefix)
        student = (window_sum + lift * linear_sum) * inverse
        difference = student - teacher[h * ROWS : (h + 1) * ROWS]
        square = difference * difference
        for k in range(ROWS // 8):
            loss = loss + square[k * 8 : (k + 1) * 8]
        grad_out = difference * (2.0 / TOKENS)
        num_grad = lift * grad_out * inverse
        den_grad = -lift * jnp.sum(grad_out * student, axis=1, keepdims=True) * inverse
        dgt = den_grad.T
        adjoint.append(dot_wide(qft, num_grad))
        a_column.append(jnp.sum(qft * dgt[:1], axis=1, keepdims=True))
        kept.append((prefix, num_grad, dgt))
    tile[...] = loss
    for p in others:
        remote(tile, tiles.at[xx], send.at[3], recv.at[3, xx], X, p).start()
    tiles[xx] = loss

    def start(k, axis, src, dst):
        for d in FAR_FIRST:
            p = around(place[axis], d)
            remote(src(p), dst.at[place[axis]], send.at[k], recv.at[k, place[axis]], axis, p).start()

    def finish(k, axis, dst):
        for d in NEAR_FIRST:
            p = around(place[axis], d)
            remote(dst.at[p], dst.at[p], send.at[k], recv.at[k, p], axis, p).wait_recv()

    def added(ref, low=0, high=RING):
        out = ref[low]
        for k in range(low + 1, high):
            out = out + ref[k]
        return out

    near = []
    for h in range(2):
        q, qft, qf, kft, prefix_sum = heads[h][:5]
        prefix, num_grad, dgt = kept[h]
        ngt = num_grad.T
        link = jnp.where(turned_mask, dot_right(vext, ngt) + dgt[:1], 0.0)
        qfg = dot_wide(kft, link) + dot_wide(prefix, ngt) + prefix_sum * dgt[:1]
        kfg = dot_wide(qft, link, NT)
        grad_query = dot_left(features_back(qft, qfg), q)
        queries[h] = grad_query
        near.append(dot_left(features_back(kft, kfg), kext))
    far[...] = jnp.zeros_like(far)
    work = functools.partial(
        on_grads, two(jnp.concatenate(adjoint, axis=0)), jnp.concatenate(a_column, axis=0)
    )
    lines(0, work)
    lines(1, work)
    for h in range(2):
        for k in range(4):
            g[4 * h + k] = queries[h][16 * k : 16 * (k + 1)]
    start(0, Z, lambda p: g.at[p], g1)
    g1[z] = g[z]
    for hop in range(2, 5):
        lines(hop, work)
    far[...] += jnp.concatenate(near, axis=0)
    for h in range(2):
        for k in range(RING):
            gk[h, k] = far[h * HALF + 8 * k : h * HALF + 8 * (k + 1)]

    ways = ((Y, Z, y, z), (Z, Y, z, y))
    for h, (one, other, mine, across) in enumerate(ways):
        start(6 + h, one, lambda p, h=h: gk.at[h, p], k1.at[h])
        k1[h, mine] = gk[h, mine]
    for p in others:
        remote(tile, tiles.at[p], send.at[3], recv.at[3, p], X, p).wait_recv()
    tile_x[...] = added(tiles, 0, 4)
    start(4, Z, lambda p: tile_x, l1)
    l1[z] = tile_x[...]
    finish(0, Z, g1)
    g1s[...] = added(g1)
    start(1, Y, lambda p: g1s, g2)
    g2[y] = g1s[...]
    for h, (one, other, mine, across) in enumerate(ways):
        finish(6 + h, one, k1.at[h])
        k1s[h] = added(k1[h])
        start(8 + h, other, lambda p, h=h: k1s.at[h], k2.at[h])
        k2[h, across] = k1s[h]
    finish(4, Z, l1)
    l1s[...] = added(l1)
    start(5, Y, lambda p: l1s, l2)
    l2[y] = l1s[...]
    finish(1, Y, g2)
    g2s[...] = added(g2)
    start(2, Z, lambda p: g2s, out_g)
    out_g[z] = g2s[...]
    for h, (one, other, mine, across) in enumerate(ways):
        finish(8 + h, other, k2.at[h])
        k2s[h] = added(k2[h])
        start(10 + h, one, lambda p, h=h: k2s.at[h], out_k.at[h])
        out_k[h, mine] = k2s[h]
    finish(5, Y, l2)
    out_loss[...] = added(l2)
    finish(2, Z, out_g)
    for h, (one, other, mine, across) in enumerate(ways):
        finish(10 + h, one, out_k.at[h])

    for stream in k_streams + v_streams:
        sent = stream[0].at[pl.ds(0, RING * RING - 1)]
        remote(sent, sent, stream[1], stream[2].at[0], Z, z).wait_send()
    for k, ref, count in (
        (0, g1, 7), (1, g2, 7), (2, out_g, 7), (3, tiles, 3), (4, l1, 7), (5, l2, 7),
        (6, k1.at[0], 7), (7, k1.at[1], 7), (8, k2.at[0], 7), (9, k2.at[1], 7),
        (10, out_k.at[0], 7), (11, out_k.at[1], 7),
    ):
        sent = ref.at[pl.ds(0, count)]
        remote(sent, sent, send.at[k], recv.at[k, 0], Z, z).wait_send()


VMEM = pl.BlockSpec(memory_space=pltpu.VMEM)


def layer(queries, keys, values, query_weight, key_weight):
    shape = jax.ShapeDtypeStruct
    dma = pltpu.SemaphoreType.DMA

    def f32(*dims):
        return pltpu.VMEM(dims, F32)

    def bf16(*dims):
        return pltpu.VMEM(dims, BF16)

    blocks = bf16(2 * RING * RING, HALF, 128)
    scratch = [
        blocks, blocks, f32(16, 256, LINE), bf16(16, 256, LINE), bf16(16, 256, LINE),
        f32(256, 128), f32(256, 128), f32(256, 128), f32(256, 128), f32(256, 128),
        f32(128, 128), f32(8, 16, 128), f32(8, 16, 128), f32(16, 128), f32(8, 16, 128), f32(16, 128),
        f32(8, 128), f32(4, 8, 128), f32(8, 128), f32(8, 8, 128), f32(8, 128), f32(8, 8, 128),
        f32(2, 8, 8, 128), f32(2, 8, 8, 128), f32(2, 8, 128), f32(2, 8, 8, 128), f32(2, 8, 128),
        dma((4,)), dma((128,)), dma((128,)), dma((12,)), dma((12, RING)),
    ]
    return pl.pallas_call(
        layer_kernel,
        out_shape=(shape((8, 16, 128), F32), shape((2, 8, 8, 128), F32), shape((8, 128), F32)),
        in_specs=[VMEM] * 5,
        out_specs=(VMEM,) * 3,
        scratch_shapes=scratch,
        compiler_params=pltpu.CompilerParams(
            collective_id=0, has_side_effects=True, vmem_limit_bytes=60 * 1024 * 1024
        ),
        name="layer",
    )(queries, keys, values, query_weight, key_weight)


def finish_kernel(g_ref, k_ref, loss_ref, loss, grad_query, grad_key):
    loss[0] = jnp.sum(loss_ref[...]) * (1.0 / TOKENS)
    grad_query[...] = g_ref[...].reshape(2, HALF, 128)
    grad_key[...] = k_ref[...].reshape(2, HALF, 128)


def local(queries, keys, values, query_weight, key_weight):
    shape = jax.ShapeDtypeStruct
    return pl.pallas_call(
        finish_kernel,
        out_shape=(
            shape((1,), F32), shape(query_weight.shape, F32), shape(key_weight.shape, F32)
        ),
        in_specs=[VMEM] * 3,
        out_specs=(pl.BlockSpec(memory_space=pltpu.SMEM), VMEM, VMEM),
        name="finish",
    )(*layer(queries, keys, values, query_weight, key_weight))


def solution(mesh):
    split = Mesh(
        mesh.devices.reshape(8, 8, mesh.shape["head"], mesh.shape["rep"]),
        (Z, Y, X, "rep"),
    )
    return jax.shard_map(
        local,
        mesh=split,
        in_specs=(
            P(REP_SEQ, X, None),
            P(REP_SEQ, None),
            P(REP_SEQ, None),
            P(("rep", X), None, None),
            P(("rep", X), None, None),
        ),
        out_specs=(P("rep"), P(("rep", X), None, None), P(("rep", X), None, None)),
        check_vma=False,
    )
```

```python
import functools

import jax
import jax.numpy as jnp
from jax import lax
from jax.experimental import pallas as pl
from jax.experimental.pallas import tpu as pltpu
from jax.sharding import Mesh
from jax.sharding import PartitionSpec as P

WINDOW = 64
Z, Y, X = "seq_0", "seq_1", "head"
REP_SEQ = ("rep", Z, Y)
MESH = pl.DeviceIdType.MESH
RING = 8
LOW = -1e30
F32 = jnp.float32
BF16 = jnp.bfloat16
FAR_FIRST = (4, 3, 5, 2, 6, 1, 7)


def around(place, steps):
    return lax.rem(place + (steps + RING), RING)


def remote(src, dst, send, recv, axis, place):
    return pltpu.make_async_remote_copy(
        src_ref=src,
        dst_ref=dst,
        send_sem=send,
        recv_sem=recv,
        device_id={axis: place},
        device_id_type=MESH,
    )


def greet(peers):
    barrier = pltpu.get_barrier_semaphore()
    for axis, place in peers:
        pl.semaphore_signal(barrier, inc=1, device_id={axis: place}, device_id_type=MESH)
    pl.semaphore_wait(barrier, len(peers))


NN = (((1,), (0,)), ((), ()))
NT = (((1,), (1,)), ((), ()))


def dot(a, b, dims=NN):
    return lax.dot_general(a, b, dims, preferred_element_type=F32)


def two(a):
    high = a.astype(BF16)
    return high, (a - high.astype(F32)).astype(BF16)


def dot_wide(a, b, dims=NN):
    a_high, a_low = two(a)
    b_high, b_low = two(b)
    return dot(a_high, b_high, dims) + (dot(a_high, b_low, dims) + dot(a_low, b_high, dims))


def dot_left(a, b, dims=NN):
    high, low = two(a)
    return dot(high, b, dims) + dot(low, b, dims)


def dot_right(a, b, dims=NN):
    high, low = two(b)
    return dot(a, high, dims) + dot(a, low, dims)


def three(a):
    high = a.astype(BF16)
    rest = a - high.astype(F32)
    mid = rest.astype(BF16)
    return high, mid, (rest - mid.astype(F32)).astype(BF16)


def features_of(pieces, tokens):
    act = sum(dot(piece, tokens, NT) for piece in pieces[1:]) + dot(pieces[0], tokens, NT)
    half = 64
    parts = []
    for h in range(act.shape[0] // half):
        one = act[h * half : (h + 1) * half]
        for e in (jnp.exp(one), jnp.exp(-one)):
            parts.append(e * (1.0 / jnp.sum(e, axis=0, keepdims=True)))
    return jnp.concatenate(parts, axis=0)


def features_back(features, grad):
    half = features.shape[0] // 2
    p, r = features[:half], features[half:]
    dp, dr = grad[:half], grad[half:]
    return p * (dp - jnp.sum(p * dp, axis=0, keepdims=True)) - r * (
        dr - jnp.sum(r * dr, axis=0, keepdims=True)
    )


def iota(shape, axis):
    return lax.broadcasted_iota(jnp.int32, shape, axis)


NEAR_FIRST = (1, 7, 2, 6, 3, 5, 4)
ROWS = 128
HALF = 64
TOKENS = ROWS * RING * RING
LINE = RING * HALF


def layer_kernel(
    q_ref, k_ref, v_ref, wq_ref, wk_ref,
    out_g, out_k, out_loss,
    kbuf, vbuf, scores, f_high, f_low, best, state, state_sum, total, accum,
    far, g, g1, g1s, g2, g2s, tile, tiles, tile_x, l1, l1s, l2, gk, k1, k1s, k2, k2s,
    kv_send, k_recv, v_recv, send, recv,
):
    z, y, xx = lax.axis_index(Z), lax.axis_index(Y), lax.axis_index(X)
    me = z * RING + y
    place = {Z: z, Y: y}
    others = [lax.rem(xx + d, 4) for d in (2, 1, 3)]
    close = [(axis, around(place[axis], d)) for d in (2, -2, 1, -1) for axis in (Z, Y)]
    greet(close + [(X, p) for p in others])

    k_streams = ((kbuf, kv_send.at[0], k_recv, 0, Y, Z), (kbuf, kv_send.at[1], k_recv, 1, Z, Y))
    v_streams = ((vbuf, kv_send.at[2], v_recv, 0, Y, Z), (vbuf, kv_send.at[3], v_recv, 1, Z, Y))

    def piece(stream, along, across):
        line = around(place[stream[5]], across)
        return (stream[3] * RING + line) * RING + around(place[stream[4]], along)

    def push(stream, src, at, axis, step):
        to = around(place[axis], step)
        remote(src, stream[0].at[at], stream[1], stream[2].at[at], axis, to).start()

    def forward(stream, at, axis, step):
        push(stream, stream[0].at[at], at, axis, step)

    def arrived(stream, at):
        block = stream[0].at[at]
        remote(block, block, stream[1], stream[2].at[at], Z, z).wait_recv()

    halves = (pl.ds(0, HALF), pl.ds(HALF, HALF))
    for stream in k_streams:
        at, src = piece(stream, 0, 0), k_ref.at[halves[stream[3]]]
        for way in (1, -1):
            push(stream, src, at, stream[5], way)
    for ref, streams in ((k_ref, k_streams), (v_ref, v_streams)):
        for step in (1, -1, 2, -2):
            for stream in streams:
                push(stream, ref.at[halves[stream[3]]], piece(stream, 0, 0), stream[4], step)
    for stream in v_streams:
        at, src = piece(stream, 0, 0), v_ref.at[halves[stream[3]]]
        for way in (1, -1):
            push(stream, src, at, stream[5], way)

    for ref, streams in ((k_ref, k_streams), (v_ref, v_streams)):
        for stream in streams:
            stream[0][piece(stream, 0, 0)] = ref[halves[stream[3]]]
    best[...] = jnp.full(best.shape, LOW, F32)
    for ref in (state, state_sum, total, accum):
        ref[...] = jnp.zeros_like(ref)
    queries = [q_ref[:, h, :] for h in range(2)]
    q_all = jnp.concatenate(queries, axis=0)
    wk = three(wk_ref[...].reshape(2 * HALF, 128))

    query_features = []
    for h in range(2):
        qft = features_of(three(wq_ref[h]), queries[h])
        query_features.append((qft, qft.T))

    for offsets in ((-1, 1, -2, 2), (-3, 3, 4)):
        for streams in (k_streams, v_streams):
            for along in offsets:
                for stream in streams:
                    at = piece(stream, along, 0)
                    arrived(stream, at)
                    if along == -2:
                        forward(stream, at, stream[4], 1)
                        if streams is k_streams:
                            forward(stream, at, stream[4], 2)
                    if along == 2:
                        forward(stream, at, stream[4], -1)
                        if streams is v_streams:
                            forward(stream, at, stream[4], -2)
                    forward(stream, at, stream[5], 1)
                    forward(stream, at, stream[5], -1)

    def pass_on(streams, hop):
        for along in (0, -1, 1, -2, 2, -3, 3, 4):
            for way in (1, -1):
                last = (way == 1) == (along % 2 == 0)
                if hop == 4 and not last:
                    continue
                for stream in streams:
                    at = piece(stream, along, -way * hop)
                    arrived(stream, at)
                    if hop < 3 or (hop == 3 and last):
                        forward(stream, at, stream[5], way)

    first = me * ROWS
    bound = first - WINDOW
    scale = 128 ** (-0.5)
    lane = iota((1, LINE), 1)
    lane_block, lane_row = jnp.right_shift(lane, 6), jnp.bitwise_and(lane, HALF - 1)
    query_place = first + jnp.bitwise_and(iota((2 * ROWS, 1), 0), ROWS - 1)

    def lanes(fold, start, value):
        for k in range(LINE // 128):
            start = fold(start, value[:, k * 128 : (k + 1) * 128])
        return start

    def chunk(buf, c):
        return buf[pl.ds(c * RING, RING)].reshape(LINE, 128)

    def on_keys(cs):
        top, sums = best[...], state_sum[...]
        for c in cs:
            line = jnp.bitwise_and(c, RING - 1)
            second = c >= RING
            at = jnp.where(second, line * ROWS + HALF, line * (ROWS * RING))
            at = at + lane_block * jnp.where(second, ROWS * RING, ROWS) + lane_row
            kc = chunk(kbuf, c)
            s = dot(q_all, kc, NT) * scale
            s = jnp.where(at <= query_place, s, LOW)
            scores[c] = s
            top = lanes(jnp.maximum, top, s)
            f = jnp.where(at < bound, features_of(wk[:2], kc), 0.0)
            sums = lanes(jnp.add, sums, f)
            f_high[c], f_low[c] = two(f)
        best[...], state_sum[...] = top, sums

    def on_state(cs):
        add = state[...]
        for c in cs:
            vc = chunk(vbuf, c)
            add = add + (dot(f_high[c], vc) + dot(f_low[c], vc))
        state[...] = add

    def on_weights(top, cs):
        sums, add = total[...], accum[...]
        for c in cs:
            w = jnp.exp(scores[c] - top)
            sums = lanes(jnp.add, sums, w)
            add = add + dot(w.astype(BF16), chunk(vbuf, c))
        total[...], accum[...] = sums, add

    def on_grads(adjoint, a_column, cs):
        add = far[...]
        for c in cs:
            vc = chunk(vbuf, c)
            grad = dot(adjoint[0], vc, NT) + dot(adjoint[1], vc, NT) + a_column
            f = f_high[c].astype(F32) + f_low[c].astype(F32)
            back = [features_back(f[i : i + ROWS], grad[i : i + ROWS]) for i in (0, ROWS)]
            add = add + dot_left(jnp.concatenate(back, axis=0), chunk(kbuf, c))
        far[...] = add

    def lines(hop, work):
        ways = (hop,) if hop in (0, 4) else (-hop, hop)
        work([c for way in ways for c in (around(z, way), RING + around(y, way))])

    before = jnp.where(y > 0, (RING + y - 1) * RING + z, (2 * RING - 1) * RING + jnp.maximum(z - 1, 0))
    tt, jj = iota((ROWS, 2 * ROWS), 0), iota((ROWS, 2 * ROWS), 1)
    window = (jj > tt) & (jj <= tt + WINDOW) & (bound + jj >= 0)
    tt, jj = iota((ROWS, ROWS), 0), iota((ROWS, ROWS), 1)
    linear_mask = (jj <= tt) & (bound + jj >= 0)
    turned_mask = (tt <= jj) & (bound + tt >= 0)

    def nearby(h):
        kext = jnp.concatenate([kbuf[before], k_ref[...], k_ref[pl.ds(HALF, HALF)]], axis=0)
        q = queries[h]
        s = dot(q, kext, NT) * scale
        window_best = jnp.max(jnp.where(window, s, LOW), axis=1, keepdims=True)
        weights = jnp.where(window, jnp.exp(s - window_best), 0.0)
        window_total = jnp.sum(weights, axis=1, keepdims=True)
        qft, qf = query_features[h]
        kft = features_of([w[h * HALF : (h + 1) * HALF] for w in wk], kext[:ROWS])
        linear = jnp.where(linear_mask, dot_wide(qf, kft), 0.0)
        linear_total = jnp.sum(linear, axis=1, keepdims=True)
        lift = jnp.exp(-window_best)
        return q, weights.astype(BF16), window_total, qft, qf, kft, linear, linear_total, lift

    def ready(h, head):
        q, weights, window_total, qft, qf, kft, linear, linear_total, lift = head
        vext = jnp.concatenate([vbuf[before], v_ref[...], v_ref[pl.ds(HALF, HALF)]], axis=0)
        prefix_sum = jnp.sum(state_sum[h * ROWS : (h + 1) * ROWS, :], axis=1, keepdims=True)
        linear_total = linear_total + dot_wide(qf, jnp.broadcast_to(prefix_sum, (128, 128)))
        inverse = 1.0 / (window_total + lift * linear_total)
        return q, qft, qf, kft, prefix_sum, lift, inverse, dot(weights, vext), dot_left(linear, vext[:ROWS])

    heads = []
    lines(0, on_keys)
    lines(0, on_state)
    for hop in (1, 2, 3):
        pass_on(k_streams, hop)
        pass_on(v_streams, hop)
        lines(hop, on_keys)
        lines(hop, on_state)
        if hop < 3:
            heads.append(nearby(hop - 1))
    pass_on(k_streams, 4)
    lines(4, on_keys)
    top = jnp.max(best[...], axis=1, keepdims=True)
    on_weights = functools.partial(on_weights, top)
    for hop in range(4):
        lines(hop, on_weights)
    heads = [ready(h, heads[h]) for h in range(2)]
    pass_on(v_streams, 4)
    lines(4, on_state)
    lines(4, on_weights)

    kext = jnp.concatenate([kbuf[before], k_ref[pl.ds(0, HALF)]], axis=0)
    vext = jnp.concatenate([vbuf[before], v_ref[pl.ds(0, HALF)]], axis=0)
    teacher = accum[...] / jnp.sum(total[...], axis=1, keepdims=True)
    teacher = teacher.astype(BF16).astype(F32)
    loss = jnp.zeros((8, 128), F32)
    kept, adjoint, a_column = [], [], []
    for h in range(2):
        q, qft, qf, kft, prefix_sum, lift, inverse, window_sum, linear_sum = heads[h]
        prefix = state[h * ROWS : (h + 1) * ROWS, :]
        linear_sum = linear_sum + dot_wide(qf, prefix)
        student = (window_sum + lift * linear_sum) * inverse
        difference = student - teacher[h * ROWS : (h + 1) * ROWS]
        square = difference * difference
        for k in range(ROWS // 8):
            loss = loss + square[k * 8 : (k + 1) * 8]
        grad_out = difference * (2.0 / TOKENS)
        num_grad = lift * grad_out * inverse
        den_grad = -lift * jnp.sum(grad_out * student, axis=1, keepdims=True) * inverse
        dgt = den_grad.T
        adjoint.append(dot_wide(qft, num_grad))
        a_column.append(jnp.sum(qft * dgt[:1], axis=1, keepdims=True))
        kept.append((prefix, num_grad, dgt))
    tile[...] = loss
    for p in others:
        remote(tile, tiles.at[xx], send.at[3], recv.at[3, xx], X, p).start()
    tiles[xx] = loss

    def start(k, axis, src, dst):
        for d in FAR_FIRST:
            p = around(place[axis], d)
            remote(src(p), dst.at[place[axis]], send.at[k], recv.at[k, place[axis]], axis, p).start()

    def finish(k, axis, dst):
        for d in NEAR_FIRST:
            p = around(place[axis], d)
            remote(dst.at[p], dst.at[p], send.at[k], recv.at[k, p], axis, p).wait_recv()

    def added(ref, low=0, high=RING):
        out = ref[low]
        for k in range(low + 1, high):
            out = out + ref[k]
        return out

    near = []
    for h in range(2):
        q, qft, qf, kft, prefix_sum = heads[h][:5]
        prefix, num_grad, dgt = kept[h]
        ngt = num_grad.T
        link = jnp.where(turned_mask, dot_right(vext, ngt) + dgt[:1], 0.0)
        qfg = dot_wide(kft, link) + dot_wide(prefix, ngt) + prefix_sum * dgt[:1]
        kfg = dot_wide(qft, link, NT)
        grad_query = dot_left(features_back(qft, qfg), q)
        queries[h] = grad_query
        near.append(dot_left(features_back(kft, kfg), kext))
    far[...] = jnp.zeros_like(far)
    work = functools.partial(
        on_grads, two(jnp.concatenate(adjoint, axis=0)), jnp.concatenate(a_column, axis=0)
    )
    lines(0, work)
    lines(1, work)
    for h in range(2):
        for k in range(4):
            g[4 * h + k] = queries[h][16 * k : 16 * (k + 1)]
    start(0, Z, lambda p: g.at[p], g1)
    g1[z] = g[z]
    for hop in range(2, 5):
        lines(hop, work)
    far[...] += jnp.concatenate(near, axis=0)
    for h in range(2):
        for k in range(RING):
            gk[h, k] = far[h * HALF + 8 * k : h * HALF + 8 * (k + 1)]

    ways = ((Y, Z, y, z), (Z, Y, z, y))
    for h, (one, other, mine, across) in enumerate(ways):
        start(6 + h, one, lambda p, h=h: gk.at[h, p], k1.at[h])
        k1[h, mine] = gk[h, mine]
    for p in others:
        remote(tile, tiles.at[p], send.at[3], recv.at[3, p], X, p).wait_recv()
    tile_x[...] = added(tiles, 0, 4)
    start(4, Z, lambda p: tile_x, l1)
    l1[z] = tile_x[...]
    finish(0, Z, g1)
    g1s[...] = added(g1)
    start(1, Y, lambda p: g1s, g2)
    g2[y] = g1s[...]
    for h, (one, other, mine, across) in enumerate(ways):
        finish(6 + h, one, k1.at[h])
        k1s[h] = added(k1[h])
        start(8 + h, other, lambda p, h=h: k1s.at[h], k2.at[h])
        k2[h, across] = k1s[h]
    finish(4, Z, l1)
    l1s[...] = added(l1)
    start(5, Y, lambda p: l1s, l2)
    l2[y] = l1s[...]
    finish(1, Y, g2)
    g2s[...] = added(g2)
    start(2, Z, lambda p: g2s, out_g)
    out_g[z] = g2s[...]
    for h, (one, other, mine, across) in enumerate(ways):
        finish(8 + h, other, k2.at[h])
        k2s[h] = added(k2[h])
        start(10 + h, one, lambda p, h=h: k2s.at[h], out_k.at[h])
        out_k[h, mine] = k2s[h]
    finish(5, Y, l2)
    out_loss[...] = added(l2)
    finish(2, Z, out_g)
    for h, (one, other, mine, across) in enumerate(ways):
        finish(10 + h, one, out_k.at[h])

    for stream in k_streams + v_streams:
        sent = stream[0].at[pl.ds(0, RING * RING - 1)]
        remote(sent, sent, stream[1], stream[2].at[0], Z, z).wait_send()
    for k, ref, count in (
        (0, g1, 7), (1, g2, 7), (2, out_g, 7), (3, tiles, 3), (4, l1, 7), (5, l2, 7),
        (6, k1.at[0], 7), (7, k1.at[1], 7), (8, k2.at[0], 7), (9, k2.at[1], 7),
        (10, out_k.at[0], 7), (11, out_k.at[1], 7),
    ):
        sent = ref.at[pl.ds(0, count)]
        remote(sent, sent, send.at[k], recv.at[k, 0], Z, z).wait_send()


VMEM = pl.BlockSpec(memory_space=pltpu.VMEM)


def layer(queries, keys, values, query_weight, key_weight):
    shape = jax.ShapeDtypeStruct
    dma = pltpu.SemaphoreType.DMA

    def f32(*dims):
        return pltpu.VMEM(dims, F32)

    def bf16(*dims):
        return pltpu.VMEM(dims, BF16)

    blocks = bf16(2 * RING * RING, HALF, 128)
    scratch = [
        blocks, blocks, f32(16, 256, LINE), bf16(16, 256, LINE), bf16(16, 256, LINE),
        f32(256, 128), f32(256, 128), f32(256, 128), f32(256, 128), f32(256, 128),
        f32(128, 128), f32(8, 16, 128), f32(8, 16, 128), f32(16, 128), f32(8, 16, 128), f32(16, 128),
        f32(8, 128), f32(4, 8, 128), f32(8, 128), f32(8, 8, 128), f32(8, 128), f32(8, 8, 128),
        f32(2, 8, 8, 128), f32(2, 8, 8, 128), f32(2, 8, 128), f32(2, 8, 8, 128), f32(2, 8, 128),
        dma((4,)), dma((128,)), dma((128,)), dma((12,)), dma((12, RING)),
    ]
    return pl.pallas_call(
        layer_kernel,
        out_shape=(shape((8, 16, 128), F32), shape((2, 8, 8, 128), F32), shape((8, 128), F32)),
        in_specs=[VMEM] * 5,
        out_specs=(VMEM,) * 3,
        scratch_shapes=scratch,
        compiler_params=pltpu.CompilerParams(
            collective_id=0, has_side_effects=True, vmem_limit_bytes=60 * 1024 * 1024
        ),
        name="layer",
    )(queries, keys, values, query_weight, key_weight)


def finish_kernel(g_ref, k_ref, loss_ref, loss, grad_query, grad_key):
    loss[0] = jnp.sum(loss_ref[...]) * (1.0 / TOKENS)
    grad_query[...] = g_ref[...].reshape(2, HALF, 128)
    grad_key[...] = k_ref[...].reshape(2, HALF, 128)


def local(queries, keys, values, query_weight, key_weight):
    shape = jax.ShapeDtypeStruct
    return pl.pallas_call(
        finish_kernel,
        out_shape=(
            shape((1,), F32), shape(query_weight.shape, F32), shape(key_weight.shape, F32)
        ),
        in_specs=[VMEM] * 3,
        out_specs=(pl.BlockSpec(memory_space=pltpu.SMEM), VMEM, VMEM),
        name="finish",
    )(*layer(queries, keys, values, query_weight, key_weight))


def solution(mesh):
    split = Mesh(
        mesh.devices.reshape(8, 8, mesh.shape["head"], mesh.shape["rep"]),
        (Z, Y, X, "rep"),
    )
    return jax.shard_map(
        local,
        mesh=split,
        in_specs=(
            P(REP_SEQ, X, None),
            P(REP_SEQ, None),
            P(REP_SEQ, None),
            P(("rep", X), None, None),
            P(("rep", X), None, None),
        ),
        out_specs=(P("rep"), P(("rep", X), None, None), P(("rep", X), None, None)),
        check_vma=False,
    )
```
